32 devices in a mesh: leaf: 32 (over z, y, x, core).
Axes of the slice: x: 2, y: 2, z: 4, core: 2. Of those that a mesh axis runs over, the one named last changes fastest.
Arguments:
- points: float32 [131072, 128], P('leaf')
- right_side: float32 [64, 131072], P(None, 'leaf'), may hold values from -6 to 6
- neighbours: int32 [256, 5], P('leaf'), may hold values from -1 to 255, as said below
- leaf_interp: float32 [256, 512, 256], P('leaf'), may hold values from -0.25 to 0.25
- leaf_skeleton: int32 [256, 256], P('leaf'), may hold values from 0 to 511, as said below
- node_skeleton: int32 [254, 256], replicated, may hold values from 0 to 511, as said below
- node_gain: float32 [510, 256], replicated, may hold values from 0.5 to 1.5
- transfer: float32 [7, 2, 256, 256], replicated, may hold values from -0.1875 to 0.1875
Outputs:
- solution: float32 [64, 131072], P(None, 'leaf')
- residual: float32 [64, 131072], P(None, 'leaf')
The draws below stay inside these ranges and needn't reach their ends.
Inputs may be any that keep to these rules, and one draw needn't show every extreme that they name: `neighbours`: slot s of leaf j holds j + s - 2 or -1, and slot 2 holds j; leaf m stands in leaf j's list exactly when j stands in leaf m's. `leaf_skeleton`: the entries of a row are distinct. `node_skeleton`: the entries of a row are distinct.
All inputs are finite; a program needn't handle non-finite values.
Results may differ from the reference program's by a relative error of at most 0.0003.
Values sent between devices are 32-bit elements; how exact they have to be, the bound alone decides.
No kernel may reach another device: no remote copies, remote signals or barrier semaphores. Data moves between devices by JAX's collectives and lax.ppermute only.
A program may use at most 192 MiB of HBM per device.

```python
import math
import jax
import jax.numpy as jnp
from jax import lax

LEAF = 512
SKEL = 256
DIM = 128
CLASSES = 64
RANGE = 2
ITERS = 2
LEVELS = 8
LEAVES = 256
POINTS = 131072


latent_dims = 8


def draw_points(key, part):
    embedding = jax.random.normal(jax.random.fold_in(key, 3000), (latent_dims, DIM), jnp.float32) * DIM ** (-0.5)
    centres = jnp.zeros((LEAVES, latent_dims), jnp.float32)
    for level in range(LEVELS + 1):
        offsets = jax.random.normal(jax.random.fold_in(key, level + 1), (LEAVES >> level, latent_dims), jnp.float32)
        centres = centres + 0.15 * jnp.repeat(offsets, 2 ** level, axis=0)
    radius = jnp.exp(jax.random.uniform(jax.random.fold_in(key, 1000), (LEAVES, LEAF, 1), jnp.float32, jnp.log(0.6), 0.0))
    latent = jax.random.normal(jax.random.fold_in(key, 2000), (LEAVES, LEAF, latent_dims), jnp.float32)
    located = centres[:, None, :] + radius * latent
    embedded = jnp.einsum('nqk,kd->nqd', located, embedding, precision=lax.Precision.HIGHEST)
    ambient = jax.random.normal(jax.random.fold_in(key, 4000), (LEAVES, LEAF, DIM), jnp.float32) * DIM ** (-0.5)
    return (embedded + ambient).reshape(POINTS, DIM)


def draw_neighbours(key, part):
    leaf_ids = jnp.arange(LEAVES, dtype=jnp.int32)
    links = jax.random.randint(key, (LEAVES, RANGE), 0, 4) > 0
    columns = []
    for offset in range(RANGE, 0, -1):
        lower = leaf_ids - offset
        linked = jnp.roll(links[:, offset - 1], offset) & (lower >= 0)
        columns.append(jnp.where(linked, lower, -1))
    columns.append(leaf_ids)
    for offset in range(1, RANGE + 1):
        upper = leaf_ids + offset
        linked = links[:, offset - 1] & (upper < LEAVES)
        columns.append(jnp.where(linked, upper, -1))
    return jnp.stack(columns, axis=1).astype(jnp.int32)


def distinct_rows(key, row_count, width, chosen):
    scores = jax.random.randint(key, (row_count, width), 0, 1 << 20) * width + jnp.arange(width, dtype=jnp.int32)[None, :]
    order = jnp.argsort(scores, axis=1)
    return order[:, :chosen].astype(jnp.int32)


def draw_leaf_skeleton(key, part):
    return distinct_rows(jax.random.fold_in(key, 11), LEAVES, LEAF, SKEL)


def draw_node_skeleton(key, part):
    return distinct_rows(jax.random.fold_in(key, 12), LEAVES - 2, 2 * SKEL, SKEL)


def block_levels(own_key, extent, cuts, smallest, largest):
    def one(dim, blocks):
        steps = jax.random.uniform(jax.random.fold_in(jax.random.fold_in(own_key, 6), dim), (blocks,), jnp.float32, smallest / len(cuts), largest / len(cuts))
        return jnp.repeat(jnp.exp(steps), extent[dim] // blocks).reshape((-1,) + (1,) * (len(extent) - dim - 1))

    loudness = one(*cuts[0])
    for cut in cuts[1:]:
        loudness = loudness * one(*cut)
    return loudness


def noise(key, shape, deviation, bound, cuts=(), kind=jnp.bfloat16):
    gain = block_levels(key, shape, cuts, -0.22, 0.18) if cuts else 1.0
    entries = jax.random.normal(key, shape, jnp.float32) * deviation * gain
    return jnp.minimum(jnp.maximum(entries, -bound), bound).astype(kind)


def setup_inputs(seed: int = 0) -> dict:
    arg_keys = jax.random.split(jax.random.key(seed), 9)
    points = draw_points(jax.random.fold_in(arg_keys[8], 71), 0)
    right_side = noise(arg_keys[1], (CLASSES, POINTS), 1.0, 6.0, ((1, 32),), jnp.float32)
    neighbours = draw_neighbours(jax.random.fold_in(arg_keys[8], 71), 0)
    leaf_interp = noise(arg_keys[3], (LEAVES, LEAF, SKEL), LEAF ** -0.5, 0.25, ((0, 32),), jnp.float32)
    leaf_skeleton = draw_leaf_skeleton(jax.random.fold_in(arg_keys[8], 71), 0)
    node_skeleton = draw_node_skeleton(jax.random.fold_in(arg_keys[8], 71), 0)
    node_gain = jnp.clip(jnp.exp(jax.random.uniform(arg_keys[6], (2 * LEAVES - 2, SKEL), jnp.float32, math.log(0.5), math.log(1.5))), 0.5, 1.5)
    transfer = noise(arg_keys[7], (LEVELS - 1, 2, SKEL, SKEL), (4 * SKEL) ** -0.5, 0.1875, (), jnp.float32)
    return {"points": points, "right_side": right_side, "neighbours": neighbours, "leaf_interp": leaf_interp, "leaf_skeleton": leaf_skeleton, "node_skeleton": node_skeleton, "node_gain": node_gain, "transfer": transfer}


highest = lax.Precision.HIGHEST
ridge = 1.0

def pair_kernel(first_set, second_set):
    inner = jnp.einsum('nqd,npd->nqp', first_set, second_set, precision=highest)
    first_norm = jnp.sum(first_set * first_set, axis=-1)
    second_norm = jnp.sum(second_set * second_set, axis=-1)
    return jnp.exp((2.0 * inner - first_norm[:, :, None] - second_norm[:, None, :]) * 0.5)

def symmetric(matrix):
    return 0.5 * (matrix + matrix.T)

def chol_apply(matrix, target):
    factor = jnp.linalg.cholesky(matrix)
    return jax.scipy.linalg.cho_solve((factor, True), target)

def reference(points, right_side, neighbours, leaf_interp, leaf_skeleton, node_skeleton, node_gain, transfer):
    coords = points.reshape(LEAVES, LEAF, DIM)
    near_mask = (neighbours >= 0).astype(jnp.float32)
    padded_coords = jnp.pad(coords, ((RANGE, RANGE), (0, 0), (0, 0)))
    skel_points = jnp.take_along_axis(coords, leaf_skeleton[:, :, None], axis=1)
    far_tiles = []
    for level in range(LEVELS):
        node_count = LEAVES >> level
        paired = skel_points.reshape(node_count // 2, 2, SKEL, DIM)
        sibling = paired[:, ::-1].reshape(node_count, SKEL, DIM)
        far_tiles.append(pair_kernel(sibling, skel_points))
        if level + 1 < LEVELS:
            first_row = LEAVES - 2 * (LEAVES >> level + 1)
            picked = node_skeleton[first_row:first_row + node_count // 2]
            skel_points = jnp.take_along_axis(paired.reshape(node_count // 2, 2 * SKEL, DIM), picked[:, :, None], axis=1)

    def gains_of(level):
        first_row = 2 * LEAVES - 2 * (LEAVES >> level)
        return node_gain[first_row:first_row + (LEAVES >> level)]

    def sibling_of(values):
        node_count = values.shape[0]
        return values.reshape(node_count // 2, 2, CLASSES, SKEL)[:, ::-1].reshape(node_count, CLASSES, SKEL)

    def operate(vector):
        by_leaf = vector.reshape(CLASSES, LEAVES, LEAF).transpose(1, 0, 2)
        padded_rows = jnp.pad(by_leaf, ((RANGE, RANGE), (0, 0), (0, 0)))

        def near_leaf(leaf_id):
            own_coords = lax.dynamic_index_in_dim(padded_coords, leaf_id + RANGE, 0, keepdims=False)
            total = jnp.zeros((CLASSES, LEAF), jnp.float32)
            for slot_id in range(2 * RANGE + 1):
                other_coords = lax.dynamic_index_in_dim(padded_coords, leaf_id + slot_id, 0, keepdims=False)
                other_rows = lax.dynamic_index_in_dim(padded_rows, leaf_id + slot_id, 0, keepdims=False)
                tile = pair_kernel(other_coords[None], own_coords[None])[0]
                total = total + near_mask[leaf_id, slot_id] * jnp.dot(other_rows, tile, precision=highest)
            return total
        near = lax.map(near_leaf, jnp.arange(LEAVES, dtype=jnp.int32))
        weights = jnp.einsum('ncq,nqs->ncs', by_leaf, leaf_interp, precision=highest)
        weight_levels = [weights]
        for level in range(LEVELS - 1):
            node_count = LEAVES >> level
            scaled = weights.reshape(node_count // 2, 2, CLASSES, SKEL) * gains_of(level).reshape(node_count // 2, 2, 1, SKEL)
            weights = jnp.einsum('ncs,st->nct', scaled[:, 0], transfer[level, 0], precision=highest)
            weights = weights + jnp.einsum('ncs,st->nct', scaled[:, 1], transfer[level, 1], precision=highest)
            weight_levels.append(weights)
        top = LEVELS - 1
        potential = jnp.einsum('ncs,nst->nct', sibling_of(weight_levels[top]), far_tiles[top], precision=highest)
        for level in range(LEVELS - 2, -1, -1):
            node_count = LEAVES >> level
            children = jnp.stack([jnp.einsum('nct,st->ncs', potential, transfer[level, 0], precision=highest), jnp.einsum('nct,st->ncs', potential, transfer[level, 1], precision=highest)], axis=1)
            children = children.reshape(node_count, CLASSES, SKEL) * gains_of(level)[:, None, :]
            potential = children + jnp.einsum('ncs,nst->nct', sibling_of(weight_levels[level]), far_tiles[level], precision=highest)
        far = jnp.einsum('ncs,nqs->ncq', potential, leaf_interp, precision=highest)
        near_flat = near.transpose(1, 0, 2).reshape(CLASSES, POINTS)
        far_flat = far.transpose(1, 0, 2).reshape(CLASSES, POINTS)
        return ridge * vector + near_flat + far_flat
    solution = jnp.zeros_like(right_side)
    residual = right_side
    direction = right_side
    res_norm = symmetric(jnp.dot(residual, residual.T, precision=highest))
    for step in range(ITERS):
        image = operate(direction)
        curvature = symmetric(jnp.dot(direction, image.T, precision=highest))
        alpha_mat = chol_apply(curvature, res_norm)
        solution = solution + jnp.dot(alpha_mat.T, direction, precision=highest)
        residual = residual - jnp.dot(alpha_mat.T, image, precision=highest)
        if step + 1 < ITERS:
            new_norm = symmetric(jnp.dot(residual, residual.T, precision=highest))
            beta_mat = chol_apply(res_norm, new_norm)
            direction = residual + jnp.dot(beta_mat.T, direction, precision=highest)
            res_norm = new_norm
    return (solution, residual)
```

```python
import math

import jax
import jax.numpy as jnp
from jax import lax
from jax.experimental import pallas as pl
from jax.experimental.pallas import tpu as pltpu
from jax.sharding import PartitionSpec as P

ITERS = 2
ridge = 1.0
F32 = jnp.float32
BF16 = jnp.bfloat16
COORD_SCALE = math.sqrt(math.log2(math.e))
MIB = 1024 * 1024


def nn(a, b):
    return lax.dot_general(a, b, (((1,), (0,)), ((), ())), preferred_element_type=F32)


def nt(a, b):
    return lax.dot_general(a, b, (((1,), (1,)), ((), ())), preferred_element_type=F32)


def split(x):
    hi = x.astype(BF16)
    return hi, (x - hi.astype(F32)).astype(BF16)


def stacked(x):
    return jnp.concatenate(split(x), axis=0)


def times(cat, b_hi, b_lo, mul=nn):
    rows = cat.shape[0] // 2
    both = mul(cat, b_hi)
    return both[:rows] + both[rows:] + mul(cat[:rows], b_lo)


def scaled_cat(x):
    return jnp.concatenate(split(x * COORD_SCALE), axis=1)


def half_norms(cat):
    dim = cat.shape[1] // 2
    whole = cat[:, :dim].astype(F32) + cat[:, dim:].astype(F32)
    column = 0.5 * jnp.sum(whole * whole, axis=1, keepdims=True)
    wide = jnp.broadcast_to(column, (column.shape[0], 128))
    return wide, wide.T[0:1, :]


def pair_tile(cat_a, cat_b, wide_a, row_b):
    dim = cat_b.shape[1] // 2
    b_hi, b_lo = cat_b[:, :dim], cat_b[:, dim:]
    inner = nt(
        jnp.concatenate([cat_a, cat_a], axis=1),
        jnp.concatenate([b_hi, b_hi, b_lo, b_lo], axis=1),
    )
    count = cat_b.shape[0] // 128
    return jnp.exp2(inner - jnp.concatenate([wide_a] * count, axis=1) - row_b)


def one_hot(column, width):
    rows = column.shape[0]
    spots = lax.broadcasted_iota(jnp.int32, (rows, width), 1).astype(F32)
    return jnp.where(spots == column, 1.0, 0.0).astype(BF16)


def columns(rows):
    return rows.astype(F32).T


def pack_skel(ref, first, skel):
    half = skel.shape[0] // 2
    ref[first : first + half, : skel.shape[1]] = skel[:half]
    ref[first : first + half, skel.shape[1] :] = skel[half:]


def unpack_skel(pack):
    half = pack.shape[1] // 2
    return jnp.concatenate([pack[:, :half], pack[:, half:]], axis=0)


def call(body, out_shape, name, vmem, **options):
    return pl.pallas_call(
        body,
        out_shape=out_shape,
        name=name,
        compiler_params=pltpu.CompilerParams(vmem_limit_bytes=vmem * MIB),
        **options,
    )


def struct(shape, dtype=F32):
    return jax.ShapeDtypeStruct(shape, dtype)


VM = pl.BlockSpec(memory_space=pltpu.VMEM)
SM = pl.BlockSpec(memory_space=pltpu.SMEM)


def climb_local(device, level, leaf_count, leaves, transfer_ref, gain_ref, local_ref):
    classes = level[0].shape[0]
    first, depth = 0, 0
    while len(level) > 1:
        count = len(level)
        gain_first = 2 * leaves - 2 * (leaves >> depth) + device * count
        scaled = []
        for i, weights in enumerate(level):
            local_ref[first + i] = weights
            scaled.append(weights * gain_ref[pl.ds(gain_first + i, 1), :])
        left = times(stacked(jnp.concatenate(scaled[0::2], axis=0)), *split(transfer_ref[depth, 0]))
        right = times(stacked(jnp.concatenate(scaled[1::2], axis=0)), *split(transfer_ref[depth, 1]))
        total = left + right
        first += count
        depth += 1
        level = [total[i * classes : (i + 1) * classes] for i in range(count // 2)]
    return level[0]


def leaf_weights(vector_ref, interp_ref, leaf_count, leaf_size):
    return [
        times(stacked(vector_ref[:, j * leaf_size : (j + 1) * leaf_size]), *split(interp_ref[j]))
        for j in range(leaf_count)
    ]


def front(device, points, vector, leaf_skeleton, node_skeleton, leaf_interp, transfer, node_gain, leaves):
    dim = points.shape[1]
    leaf_count, leaf_size, skel_size = leaf_interp.shape
    classes = vector.shape[0]
    pair_count = leaf_count - 1
    local_levels = leaf_count.bit_length() - 1

    def body(
        dev_ref, points_ref, vector_ref, leaf_ref, node_ref, interp_ref, transfer_ref, gain_ref,
        pack_ref, local_ref, hi_ref, lo_ref, rows_ref,
    ):
        device = dev_ref[0]
        rows_ref[...] = jnp.zeros_like(rows_ref)
        pair = 0
        for depth in range(1, local_levels + 1):
            count = leaf_count >> depth
            first = leaves - 2 * (leaves >> depth) + device * count
            for i in range(count):
                rows_ref[pair : pair + 1, :] = node_ref[pl.ds(first + i, 1), :]
                pair += 1
        leaf_columns, node_columns = columns(leaf_ref[...]), columns(rows_ref[...])
        level = []
        for j in range(leaf_count):
            cat = scaled_cat(points_ref[j * leaf_size : (j + 1) * leaf_size, :])
            level.append(nn(one_hot(leaf_columns[:, j : j + 1], leaf_size), cat).astype(BF16))
        pair = 0
        while len(level) > 1:
            above = []
            for p in range(len(level) // 2):
                left, right = level[2 * p], level[2 * p + 1]
                both = jnp.concatenate([left, right], axis=0)
                pick = one_hot(node_columns[:, pair : pair + 1], 2 * skel_size)
                above.append(nn(pick, both).astype(BF16))
                tile = pair_tile(left, right, half_norms(left)[0], half_norms(right)[1])
                hi_ref[pair], lo_ref[pair] = split(tile)
                pair += 1
            level = above
        whole = level[0]
        pack_skel(pack_ref, classes, whole[:, :dim].astype(F32) + whole[:, dim:].astype(F32))
        weights = leaf_weights(vector_ref, interp_ref, leaf_count, leaf_size)
        pack_ref[:classes] = climb_local(
            device, weights, leaf_count, leaves, transfer_ref, gain_ref, local_ref
        )

    local_maps = pl.BlockSpec((local_levels,) + transfer.shape[1:], lambda i: (0, 0, 0, 0))
    return call(
        body,
        (
            struct((classes + skel_size // 2, skel_size)),
            struct((2 * leaf_count - 2, classes, skel_size)),
            struct((pair_count, skel_size, skel_size), BF16),
            struct((pair_count, skel_size, skel_size), BF16),
        ),
        "front",
        28,
        grid=(1,),
        in_specs=[SM, VM, VM, VM, VM, VM, local_maps, VM],
        out_specs=(VM, VM, VM, VM),
        scratch_shapes=[pltpu.VMEM((leaf_count, skel_size), jnp.int32)],
    )(device, points, vector, leaf_skeleton, node_skeleton, leaf_interp, transfer, node_gain)


def upward(device, vector, gram, leaf_interp, transfer, node_gain, leaves):
    leaf_count, leaf_size, skel_size = leaf_interp.shape
    classes = vector.shape[0]
    local_levels = leaf_count.bit_length() - 1

    def body(dev_ref, vector_ref, gram_ref, interp_ref, transfer_ref, gain_ref, pack_ref, local_ref):
        weights = leaf_weights(vector_ref, interp_ref, leaf_count, leaf_size)
        pack_ref[:classes] = climb_local(
            dev_ref[0], weights, leaf_count, leaves, transfer_ref, gain_ref, local_ref
        )
        pack_ref[classes:] = gram_ref[...]

    local_maps = pl.BlockSpec((local_levels,) + transfer.shape[1:], lambda i: (0, 0, 0, 0))
    return call(
        body,
        (
            struct((classes + gram.shape[0], skel_size)),
            struct((2 * leaf_count - 2, classes, skel_size)),
        ),
        "upward",
        18,
        grid=(1,),
        in_specs=[SM, VM, VM, VM, local_maps, VM],
        out_specs=(VM, VM),
    )(device, vector, gram, leaf_interp, transfer, node_gain)


def apply_tile(mask, cat_a, cat_b, hi, lo, out_ref, a, b):
    out_ref[b] = out_ref[b] + mask * times(cat_a, hi, lo)
    if cat_b is not None:
        out_ref[a] = out_ref[a] + mask * times(cat_b, hi, lo, nt)


def near_build(points, vector, near_mask, leaf_count, reach):
    dim = points.shape[1]
    leaf_size = points.shape[0] // leaf_count
    classes = vector.shape[0]

    def body(points_ref, vector_ref, mask_ref, tile_ref, out_ref, cats, wides, rows, vecs):
        a = pl.program_id(0)

        @pl.when(a == 0)
        def _():
            out_ref[...] = jnp.zeros_like(out_ref)
            for j in range(leaf_count):
                cat = scaled_cat(points_ref[j * leaf_size : (j + 1) * leaf_size, :])
                cats[j] = cat
                wide, row = half_norms(cat)
                wides[j] = wide
                rows[j] = jnp.broadcast_to(row, (8, leaf_size))
                vecs[j] = stacked(vector_ref[:, j * leaf_size : (j + 1) * leaf_size])

        for step in range(reach + 1):

            @pl.when(a + step < leaf_count)
            def _():
                b = a + step
                tile = pair_tile(cats[a], cats[b], wides[a], rows[b][0:1, :])
                tile_ref[0, step, 0], tile_ref[0, step, 1] = split(tile)
                apply_tile(
                    mask_ref[a, reach + step], vecs[a], vecs[b] if step else None,
                    tile_ref[0, step, 0], tile_ref[0, step, 1], out_ref, a, b,
                )

    tile_block = pl.BlockSpec((1, reach + 1, 2, leaf_size, leaf_size), lambda a: (a, 0, 0, 0, 0))
    tiles = struct((leaf_count, reach + 1, 2, leaf_size, leaf_size), BF16)
    return call(
        body,
        (tiles, struct((leaf_count, classes, leaf_size))),
        "near_build",
        30,
        grid=(leaf_count,),
        in_specs=[
            pl.BlockSpec(points.shape, lambda a: (0, 0)),
            pl.BlockSpec(vector.shape, lambda a: (0, 0)),
            SM,
        ],
        out_specs=(
            tile_block,
            pl.BlockSpec((leaf_count, classes, leaf_size), lambda a: (0, 0, 0)),
        ),
        scratch_shapes=[
            pltpu.VMEM((leaf_count, leaf_size, 2 * dim), BF16),
            pltpu.VMEM((leaf_count, leaf_size, 128), F32),
            pltpu.VMEM((leaf_count, 8, leaf_size), F32),
            pltpu.VMEM((leaf_count, 2 * classes, leaf_size), BF16),
        ],
    )(points, vector, near_mask)


def near_apply(tiles, vector, near_mask):
    leaf_count, steps, _, leaf_size, _ = tiles.shape
    reach = steps - 1
    classes = vector.shape[0]

    def body(tile_ref, vector_ref, mask_ref, out_ref, vecs):
        a = pl.program_id(0)

        @pl.when(a == 0)
        def _():
            out_ref[...] = jnp.zeros_like(out_ref)
            for j in range(leaf_count):
                vecs[j] = stacked(vector_ref[:, j * leaf_size : (j + 1) * leaf_size])

        for step in range(steps):

            @pl.when(a + step < leaf_count)
            def _():
                b = a + step
                apply_tile(
                    mask_ref[a, reach + step], vecs[a], vecs[b] if step else None,
                    tile_ref[0, step, 0], tile_ref[0, step, 1], out_ref, a, b,
                )

    tile_block = pl.BlockSpec((1, steps, 2, leaf_size, leaf_size), lambda a: (a, 0, 0, 0, 0))
    return call(
        body,
        struct((leaf_count, classes, leaf_size)),
        "near_apply",
        20,
        grid=(leaf_count,),
        in_specs=[tile_block, pl.BlockSpec(vector.shape, lambda a: (0, 0)), SM],
        out_specs=pl.BlockSpec((leaf_count, classes, leaf_size), lambda a: (0, 0, 0)),
        scratch_shapes=[pltpu.VMEM((leaf_count, 2 * classes, leaf_size), BF16)],
    )(tiles, vector, near_mask)


def edges(leaf_count, reach):
    found = []
    for h in range(reach):
        for j in range(reach):
            offset = j - (h - reach)
            if offset <= reach:
                found.append((h, j, reach - offset))
    for h in range(reach):
        for j in range(leaf_count - reach, leaf_count):
            offset = leaf_count + h - j
            if offset <= reach:
                found.append((reach + h, j, reach + offset))
    return found


def edge_build(points, left_points, right_points, left_rows, right_rows, near_mask, leaf_count, reach):
    dim = points.shape[1]
    leaf_size = points.shape[0] // leaf_count
    classes = left_rows.shape[0]
    border = edges(leaf_count, reach)

    def body(head_ref, tail_ref, lp_ref, rp_ref, lv_ref, rv_ref, mask_ref, hi_ref, lo_ref, out_ref):
        out_ref[...] = jnp.zeros_like(out_ref)
        for t, (h, j, slot) in enumerate(border):
            hs, hv = (lp_ref, lv_ref) if h < reach else (rp_ref, rv_ref)
            spot = h % reach
            where = slice(spot * leaf_size, (spot + 1) * leaf_size)
            cat_h = scaled_cat(hs[where, :])
            own_ref, own = (head_ref, j) if j < reach else (tail_ref, j - (leaf_count - reach))
            cat_j = scaled_cat(own_ref[own * leaf_size : (own + 1) * leaf_size, :])
            tile = pair_tile(cat_h, cat_j, half_norms(cat_h)[0], half_norms(cat_j)[1])
            hi_ref[t], lo_ref[t] = split(tile)
            spot = j if j < reach else reach + j - (leaf_count - reach)
            apply_tile(mask_ref[j, slot], stacked(hv[:, where]), None, hi_ref[t], lo_ref[t], out_ref, 0, spot)

    block = (reach * leaf_size, dim)
    last = leaf_count // reach - 1
    tiles = struct((len(border), leaf_size, leaf_size), BF16)
    return call(
        body,
        (tiles, tiles, struct((2 * reach, classes, leaf_size))),
        "edge_build",
        20,
        grid=(1,),
        in_specs=[
            pl.BlockSpec(block, lambda i: (0, 0)),
            pl.BlockSpec(block, lambda i: (last, 0)),
            VM, VM, VM, VM, SM,
        ],
        out_specs=(VM, VM, VM),
    )(points, points, left_points, right_points, left_rows, right_rows, near_mask)


def edge_apply(hi_tiles, lo_tiles, left_rows, right_rows, near_mask, leaf_count, reach):
    leaf_size = hi_tiles.shape[1]
    classes = left_rows.shape[0]
    border = edges(leaf_count, reach)

    def body(hi_ref, lo_ref, lv_ref, rv_ref, mask_ref, out_ref):
        out_ref[...] = jnp.zeros_like(out_ref)
        for t, (h, j, slot) in enumerate(border):
            hv = lv_ref if h < reach else rv_ref
            where = slice((h % reach) * leaf_size, (h % reach + 1) * leaf_size)
            spot = j if j < reach else reach + j - (leaf_count - reach)
            apply_tile(mask_ref[j, slot], stacked(hv[:, where]), None, hi_ref[t], lo_ref[t], out_ref, 0, spot)

    return call(
        body,
        struct((2 * reach, classes, leaf_size)),
        "edge_apply",
        14,
        in_specs=[VM, VM, VM, VM, SM],
        out_specs=VM,
    )(hi_tiles, lo_tiles, left_rows, right_rows, near_mask)


def tree_stage(device, packs, node_gain, transfer, node_skeleton, classes, leaves, level, bit, with_skel, extra, climb):
    count = len(packs)
    skel_size = packs[0].shape[1]
    levels = count.bit_length() - 1
    skel_rows = skel_size // 2 if with_skel else 0
    out_rows = packs[0].shape[0]

    def body(*refs):
        dev_ref, pack_refs = refs[0], refs[1 : 1 + count]
        rest = list(refs[1 + count :])
        gains_ref, transfer_ref = rest.pop(0), rest.pop(0)
        node_ref = rest.pop(0) if with_skel else None
        sibling_ref = rest.pop(0)
        next_ref = rest.pop(0)
        hi_ref, lo_ref = (rest.pop(0), rest.pop(0)) if with_skel else (None, None)
        joined = rest.pop(0)
        device = dev_ref[0]
        place = lax.shift_right_logical(device, bit) & (count - 1)
        base = lax.shift_right_logical(device, bit + levels)
        if with_skel and (climb or levels > 1):
            rows_ref = rest.pop(0)
            rows_ref[...] = jnp.zeros_like(rows_ref)
            spot = 0
            for depth in range(1, levels + 1 if climb else levels):
                nodes = count >> depth
                row = leaves - 2 * (leaves >> (level + depth)) + base * nodes
                for i in range(nodes):
                    rows_ref[spot : spot + 1, :] = node_ref[pl.ds(row + i, 1), :]
                    spot += 1
            pick_columns = columns(rows_ref[...])
        for i in range(count):
            joined[place ^ i] = pack_refs[i][...]
        weights = [joined[i][:classes] for i in range(count)]
        skels = []
        if with_skel:
            skels = [
                jnp.concatenate(split(unpack_skel(joined[i][classes : classes + skel_rows])), axis=1)
                for i in range(count)
            ]
        pick_first = 0
        for depth in range(levels):
            own = lax.shift_right_logical(place, depth)
            other = own ^ 1
            chosen = weights[0]
            for i in range(1, len(weights)):
                chosen = jnp.where(other == i, weights[i], chosen)
            sibling_ref[depth] = chosen
            if with_skel:
                mine, theirs = skels[0], skels[0]
                for i in range(1, len(skels)):
                    mine = jnp.where(own == i, skels[i], mine)
                    theirs = jnp.where(other == i, skels[i], theirs)
                tile = pair_tile(theirs, mine, half_norms(theirs)[0], half_norms(mine)[1])
                hi_ref[depth], lo_ref[depth] = split(tile)
            if depth + 1 < levels or climb:
                row = 2 * leaves - 2 * (leaves >> (level + depth)) + base * len(weights)
                scaled = [w * gains_ref[pl.ds(row + i, 1), :] for i, w in enumerate(weights)]
                left = times(stacked(jnp.concatenate(scaled[0::2], axis=0)), *split(transfer_ref[depth, 0]))
                right = times(stacked(jnp.concatenate(scaled[1::2], axis=0)), *split(transfer_ref[depth, 1]))
                total = left + right
                weights = [total[i * classes : (i + 1) * classes] for i in range(len(weights) // 2)]
                if with_skel:
                    above = []
                    for p in range(len(skels) // 2):
                        both = jnp.concatenate([skels[2 * p], skels[2 * p + 1]], axis=0)
                        pick = one_hot(pick_columns[:, pick_first : pick_first + 1], 2 * skel_size)
                        above.append(nn(pick, both).astype(BF16))
                        pick_first += 1
                    skels = above
        if climb:
            next_ref[:classes] = weights[0]
            if with_skel:
                dim = skels[0].shape[1] // 2
                pack_skel(next_ref, classes, skels[0][:, :dim].astype(F32) + skels[0][:, dim:].astype(F32))
        else:
            next_ref[: classes + skel_rows] = jnp.zeros((classes + skel_rows, skel_size), F32)
        if extra:
            rows = slice(classes + skel_rows, out_rows)
            total = joined[0][rows]
            for i in range(1, count):
                total = total + joined[i][rows]
            next_ref[rows] = total

    out = [struct((levels, classes, skel_size)), struct((out_rows, skel_size))]
    if with_skel:
        out += [struct((levels, skel_size, skel_size), BF16)] * 2
    scratch = [pltpu.VMEM((count, out_rows, skel_size), F32)]
    ins = [device, *packs, node_gain, transfer]
    if with_skel:
        ins.append(node_skeleton)
        if climb or levels > 1:
            scratch.append(pltpu.VMEM((8, skel_size), jnp.int32))
    return call(
        body,
        tuple(out),
        "tree_stage",
        10,
        in_specs=[SM] + [VM] * (len(ins) - 1),
        out_specs=tuple([VM] * len(out)),
        scratch_shapes=scratch,
    )(*ins)


def downward(
    device, vector, near, edge, leaf_interp, transfer, local_weights, local_tiles, node_gain,
    siblings, device_tiles, reach, leaves, start,
):
    leaf_count, leaf_size, skel_size = leaf_interp.shape
    classes = vector.shape[0]
    local_levels = leaf_count.bit_length() - 1
    stages = len(siblings)

    def body(*refs):
        dev_ref, vector_ref, near_ref, edge_ref, interp_hbm, transfer_hbm = refs[:6]
        weights_ref, tiles_hi, tiles_lo, gain_ref = refs[6:10]
        sib_refs = refs[10 : 10 + stages]
        dev_refs = refs[10 + stages : 10 + 3 * stages]
        rest = list(refs[10 + 3 * stages :])
        device = dev_ref[0]

        def gain(level, node):
            return gain_ref[pl.ds(2 * leaves - 2 * (leaves >> level) + node, 1), :]

        image_ref = rest.pop(0)
        head_ref, tail_ref = (rest.pop(0), rest.pop(0)) if start else (None, None)
        gram_ref = rest.pop(0) if start else None
        interp_ref, maps_ref, interp_sem, maps_sem = rest
        load_maps = pltpu.make_async_copy(transfer_hbm, maps_ref, maps_sem)
        load_interp = pltpu.make_async_copy(interp_hbm, interp_ref, interp_sem)
        load_maps.start()
        load_interp.start()
        local = []
        for s in range(stages):
            for i in range(sib_refs[s].shape[0]):
                local.append(times(stacked(sib_refs[s][i]), dev_refs[2 * s][i], dev_refs[2 * s + 1][i]))
        load_maps.wait()
        top = len(local) - 1
        potential = local[top]
        for b in range(top - 1, -1, -1):
            node = lax.shift_right_logical(device, b)
            down = maps_ref[local_levels + b, node & 1]
            potential = times(stacked(potential), *split(down), nt) * gain(local_levels + b, node) + local[b]
        level = [potential]
        for depth in range(local_levels - 1, -1, -1):
            cat = stacked(jnp.concatenate(level, axis=0))
            sides = [times(cat, *split(maps_ref[depth, c]), nt) for c in range(2)]
            count = leaf_count >> depth
            first = 2 * leaf_count - 2 * count
            pair_first = leaf_count - count
            below = []
            for n in range(count):
                p, c = n // 2, n % 2
                cat_sibling = stacked(weights_ref[first + (n ^ 1)])
                hi, lo = tiles_hi[pair_first + p], tiles_lo[pair_first + p]
                direct = times(cat_sibling, hi, lo, nn if c else nt)
                carried = sides[c][p * classes : (p + 1) * classes]
                below.append(carried * gain(depth, device * count + n) + direct)
            level = below
        load_interp.wait()
        for j in range(leaf_count):
            where = slice(j * leaf_size, (j + 1) * leaf_size)
            total = ridge * vector_ref[:, where] + near_ref[j]
            if j < reach:
                total = total + edge_ref[j]
            if j >= leaf_count - reach:
                total = total + edge_ref[reach + j - (leaf_count - reach)]
            image_ref[:, where] = total + times(stacked(level[j]), *split(interp_ref[j]), nt)
        if start:
            width = reach * leaf_size
            head_ref[...] = image_ref[:, :width]
            tail_ref[...] = image_ref[:, (leaf_count - reach) * leaf_size :]
            whole = nt(stacked(vector_ref[...]), jnp.concatenate([stacked(vector_ref[...]), stacked(image_ref[...])], axis=0))
            half = whole[:classes] + whole[classes:]
            rows = classes // 2
            self_gram = half[:, :classes] + half[:, classes : 2 * classes]
            image_gram = half[:, 2 * classes : 3 * classes] + half[:, 3 * classes :]
            gram = jnp.concatenate([self_gram, image_gram], axis=1)
            gram_ref[:, : 2 * classes] = gram[:rows]
            gram_ref[:, 2 * classes :] = gram[rows:]

    out = [struct(vector.shape)]
    if start:
        out += [struct((classes, reach * leaf_size))] * 2
        out.append(struct((classes // 2, 4 * classes)))
    ins = [device, vector, near, edge, leaf_interp, transfer, local_weights, *local_tiles, node_gain]
    ins += list(siblings)
    for pair in device_tiles:
        ins += list(pair)
    anywhere = pl.BlockSpec(memory_space=pl.ANY)
    specs = [SM, VM, VM, VM, anywhere, anywhere] + [VM] * (len(ins) - 6)
    return call(
        body,
        tuple(out),
        "downward",
        30,
        in_specs=specs,
        out_specs=tuple([VM] * len(out)),
        scratch_shapes=[
            pltpu.VMEM(leaf_interp.shape, F32),
            pltpu.VMEM(transfer.shape, F32),
            pltpu.SemaphoreType.DMA,
            pltpu.SemaphoreType.DMA,
        ],
    )(*ins)


def mixed(matrix, rows):
    m_hi, m_lo = split(matrix)
    r_hi, r_lo = split(rows)
    return nn(
        jnp.concatenate([m_hi, m_lo, m_hi, m_lo], axis=1),
        jnp.concatenate([r_hi, r_hi, r_lo, r_lo], axis=0),
    )


def three(x):
    hi = x.astype(BF16)
    rest = x - hi.astype(F32)
    mid = rest.astype(BF16)
    return hi, mid, (rest - mid.astype(F32)).astype(BF16)


def exact_dot(a, b):
    a0, a1, a2 = three(a)
    b0, b1, b2 = three(b)
    return nn(
        jnp.concatenate([a2, a1, a0, a1, a0, a0], axis=1),
        jnp.concatenate([b0, b1, b2, b0, b1, b0], axis=0),
    )


def eliminate(systems, width=4):
    size, wide = systems[0].shape
    place = lax.broadcasted_iota(jnp.int32, (size, wide), 0)
    for first in range(0, size, width):
        block = [
            [jnp.broadcast_to(m[:, k : k + 1], (size, wide)) for k in range(first, first + width)]
            for m in systems
        ]
        for i in range(width):
            k = first + i
            pivot = place == k
            for n in range(len(systems)):
                cols = block[n]
                inverse = 1.0 / cols[i][k : k + 1, :]
                for j in range(i + 1, width):
                    scaled = cols[j][k : k + 1, :] * inverse
                    cols[j] = jnp.where(pivot, scaled, cols[j] - cols[i] * scaled)
                scaled = systems[n][k : k + 1, :] * inverse
                systems[n] = jnp.where(pivot, scaled, systems[n] - cols[i] * scaled)
    return systems


def first_step(gram, right_side, image, second):
    classes = right_side.shape[0]

    def body(gram_in, b_ref, image_ref, second_ref, res_ref, res_image_ref, gram_ref, small_ref):
        packed = gram_in[classes:, :]
        both = jnp.concatenate([packed[:, : 2 * classes], packed[:, 2 * classes :]], axis=0)
        turned = both.T
        base = 0.5 * (both[:, :classes] + turned[:classes])
        curvature = 0.5 * (both[:, classes:] + turned[classes:])
        square = (classes, classes)
        unit = jnp.where(
            lax.broadcasted_iota(jnp.int32, square, 0) == lax.broadcasted_iota(jnp.int32, square, 1), 1.0, 0.0
        )
        solved, inverse = eliminate(
            [jnp.concatenate([curvature, base], axis=1), jnp.concatenate([base, unit], axis=1)]
        )
        alpha_t = solved.T[classes:]
        small_ref[:classes] = jnp.concatenate([alpha_t, inverse[:, classes:]], axis=1)
        small_ref[classes:] = both
        res = b_ref[...] - mixed(alpha_t, image_ref[...])
        res_image = image_ref[...] - mixed(alpha_t, second_ref[...])
        res_ref[...] = res
        res_image_ref[...] = res_image
        res_cat, base_cat = stacked(res), stacked(b_ref[...])
        left = jnp.concatenate([res_cat, base_cat], axis=0)
        right = jnp.concatenate([res_cat, stacked(res_image), stacked(image_ref[...])], axis=0)
        whole = nt(left, right)

        def block(i, j):
            part = whole[2 * i * classes : 2 * (i + 1) * classes, 2 * j * classes : 2 * (j + 1) * classes]
            half = part[:classes] + part[classes:]
            return half[:, :classes] + half[:, classes:]

        gram_ref[...] = jnp.concatenate([block(0, 0), block(0, 1), block(0, 2), block(1, 1)], axis=1)

    return call(
        body,
        (
            struct(right_side.shape),
            struct(right_side.shape),
            struct((classes, 4 * classes)),
            struct((2 * classes, 2 * classes)),
        ),
        "first_step",
        28,
    )(gram, right_side, image, second)


def last_step(small, parts, right_side, image, res, res_image):
    classes = right_side.shape[0]
    count = len(parts)

    def body(small_ref, *refs):
        base_ref, image_ref, res_ref, res_image_ref, sol_ref, out_ref = refs[count:]
        grams = [ref[...] for ref in refs[:count]]
        while len(grams) > 1:
            grams = [a + b for a, b in zip(grams[0::2], grams[1::2])]
        grams = grams[0]
        alpha_t = small_ref[:classes, :classes]
        inverse = small_ref[:classes, classes:]
        image_gram = small_ref[classes:, classes:]
        new_gram = grams[:, :classes]
        new_gram = 0.5 * (new_gram + grams[:, : 2 * classes].T[:classes])
        beta = exact_dot(inverse, new_gram)
        beta_t = jnp.concatenate([beta, beta], axis=1).T[:classes]
        res_image_gram = grams[:, classes : 2 * classes]
        res_base = grams[:, 2 * classes : 3 * classes]
        base_res = grams[:, 3 * classes :]
        curvature = (
            res_image_gram
            + exact_dot(res_base, beta)
            + exact_dot(beta_t, base_res + exact_dot(image_gram, beta))
        )
        curvature = 0.5 * (curvature + jnp.concatenate([curvature, curvature], axis=1).T[:classes])
        (solved,) = eliminate([jnp.concatenate([curvature, new_gram], axis=1)])
        alpha2_t = solved.T[classes:]
        direction = res_ref[...] + mixed(beta_t, base_ref[...])
        moved = res_image_ref[...] + mixed(beta_t, image_ref[...])
        sol_ref[...] = mixed(alpha_t, base_ref[...]) + mixed(alpha2_t, direction)
        out_ref[...] = res_ref[...] - mixed(alpha2_t, moved)

    return call(body, (struct(right_side.shape), struct(right_side.shape)), "last_step", 28)(
        small, *parts, right_side, image, res, res_image
    )


def body(
    points, right_side, neighbours, leaf_interp, leaf_skeleton, node_skeleton, node_gain, transfer
):
    leaf_count, slot_count = neighbours.shape
    reach = (slot_count - 1) // 2
    leaf_size, skel_size = leaf_interp.shape[1:]
    classes = right_side.shape[0]
    dev_count = lax.axis_size("leaf")
    dev_levels = dev_count.bit_length() - 1
    local_levels = leaf_count.bit_length() - 1
    levels = local_levels + dev_levels
    leaves = leaf_count * dev_count
    device = lax.axis_index("leaf").astype(jnp.int32)[None]

    def exchange(head, tail):
        ends = dev_count - 1
        left = lax.ppermute(tail, "leaf", [(i, i + 1) for i in range(ends)])
        right = lax.ppermute(head, "leaf", [(i + 1, i) for i in range(ends)])
        return left, right

    def halo(rows, axis):
        width = reach * leaf_size
        size = rows.shape[axis]
        return exchange(
            lax.slice_in_dim(rows, 0, width, axis=axis), lax.slice_in_dim(rows, size - width, size, axis=axis)
        )

    def group(pack, first_bit, count):
        return [pack] + [
            lax.ppermute(pack, "leaf", [(d, d ^ (i << first_bit)) for d in range(dev_count)])
            for i in range(1, count)
        ]

    stages = [(bit, min(2, dev_levels - bit)) for bit in range(0, dev_levels, 2)]
    near_mask = (neighbours >= 0).astype(F32)

    def climb(pack, with_skel, extra, covers):
        siblings, tiles, results = [], [], []
        for stage, (bit, width) in enumerate(stages):
            level = local_levels + bit
            depth = min(width, levels - 1 - level) or 1
            first = min(level, levels - 1 - depth)
            packs = group(pack, bit, 1 << width)
            if stage < len(covers):
                done = covers[stage](pack)
                results.append(done)
                packs, _ = lax.optimization_barrier((packs, done[-1]))
            found = tree_stage(
                device, packs, node_gain, lax.slice_in_dim(transfer, first, first + depth, axis=0),
                node_skeleton, classes, leaves, level, bit, with_skel, extra, level + width < levels,
            )
            siblings.append(found[0])
            pack = found[1]
            if with_skel:
                tiles.append((found[2], found[3]))
        return siblings, tiles, pack, results

    def after(pack, *values):
        return lax.optimization_barrier((pack, values))[1]

    left_points, right_points = halo(points, 0)
    left_rows, right_rows = halo(right_side, 1)
    pack, weights, *local_tiles = front(
        device, points, right_side, leaf_skeleton, node_skeleton, leaf_interp, transfer, node_gain, leaves
    )

    def build_near(pack):
        (vector,) = after(pack, right_side)
        return near_build(points, vector, near_mask, leaf_count, reach)

    def build_edge(pack):
        left, right = after(pack, left_rows, right_rows)
        return edge_build(points, left_points, right_points, left, right, near_mask, leaf_count, reach)

    siblings, device_tiles, _, results = climb(pack, True, False, [build_near, build_edge])
    (near_tiles, near), (edge_hi, edge_lo, edge) = results
    image, head, tail, gram = downward(
        device, right_side, near, edge, leaf_interp, transfer, weights, local_tiles, node_gain,
        siblings, device_tiles, reach, leaves, True,
    )

    left_rows, right_rows = exchange(head, tail)
    pack, weights = upward(device, image, gram, leaf_interp, transfer, node_gain, leaves)

    def apply_near(pack):
        (vector,) = after(pack, image)
        return (near_apply(near_tiles, vector, near_mask),)

    def apply_edge(pack):
        left, right = after(pack, left_rows, right_rows)
        return (edge_apply(edge_hi, edge_lo, left, right, near_mask, leaf_count, reach),)

    siblings, _, pack, results = climb(pack, False, True, [apply_near, apply_edge])
    (near,), (edge,) = results
    (second,) = downward(
        device, image, near, edge, leaf_interp, transfer, weights, local_tiles, node_gain,
        siblings, device_tiles, reach, leaves, False,
    )

    res, res_image, grams, small = first_step(pack, right_side, image, second)
    for bit, width in stages[:-1]:
        parts = group(grams, bit, 1 << width)
        while len(parts) > 1:
            parts = [a + b for a, b in zip(parts[0::2], parts[1::2])]
        grams = parts[0]
    bit, width = stages[-1]
    parts = group(grams, bit, 1 << width)
    return last_step(small, parts, right_side, image, res, res_image)


def solution(mesh):
    placed = (
        P("leaf", None),
        P(None, "leaf"),
        P("leaf", None),
        P("leaf", None, None),
        P("leaf", None),
        P(),
        P(),
        P(),
    )
    return jax.shard_map(
        body,
        mesh=mesh,
        in_specs=placed,
        out_specs=(P(None, "leaf"), P(None, "leaf")),
        check_vma=False,
    )
```

```python
import math

import jax
import jax.numpy as jnp
from jax import lax
from jax.experimental import pallas as pl
from jax.experimental.pallas import tpu as pltpu
from jax.sharding import PartitionSpec as P

ITERS = 2
ridge = 1.0
F32 = jnp.float32
BF16 = jnp.bfloat16
COORD_SCALE = math.sqrt(math.log2(math.e))
MIB = 1024 * 1024


def nn(a, b):
    return lax.dot_general(a, b, (((1,), (0,)), ((), ())), preferred_element_type=F32)


def nt(a, b):
    return lax.dot_general(a, b, (((1,), (1,)), ((), ())), preferred_element_type=F32)


def split(x):
    hi = x.astype(BF16)
    return hi, (x - hi.astype(F32)).astype(BF16)


def stacked(x):
    return jnp.concatenate(split(x), axis=0)


def times(cat, b_hi, b_lo, mul=nn):
    rows = cat.shape[0] // 2
    both = mul(cat, b_hi)
    return both[:rows] + both[rows:] + mul(cat[:rows], b_lo)


def scaled_cat(x):
    return jnp.concatenate(split(x * COORD_SCALE), axis=1)


def half_norms(cat):
    dim = cat.shape[1] // 2
    whole = cat[:, :dim].astype(F32) + cat[:, dim:].astype(F32)
    column = 0.5 * jnp.sum(whole * whole, axis=1, keepdims=True)
    wide = jnp.broadcast_to(column, (column.shape[0], 128))
    return wide, wide.T[0:1, :]


def pair_tile(cat_a, cat_b, wide_a, row_b):
    dim = cat_b.shape[1] // 2
    b_hi, b_lo = cat_b[:, :dim], cat_b[:, dim:]
    inner = nt(
        jnp.concatenate([cat_a, cat_a], axis=1),
        jnp.concatenate([b_hi, b_hi, b_lo, b_lo], axis=1),
    )
    count = cat_b.shape[0] // 128
    return jnp.exp2(inner - jnp.concatenate([wide_a] * count, axis=1) - row_b)


def one_hot(column, width):
    rows = column.shape[0]
    spots = lax.broadcasted_iota(jnp.int32, (rows, width), 1).astype(F32)
    return jnp.where(spots == column, 1.0, 0.0).astype(BF16)


def columns(rows):
    return rows.astype(F32).T


def pack_skel(ref, first, skel):
    half = skel.shape[0] // 2
    ref[first : first + half, : skel.shape[1]] = skel[:half]
    ref[first : first + half, skel.shape[1] :] = skel[half:]


def unpack_skel(pack):
    half = pack.shape[1] // 2
    return jnp.concatenate([pack[:, :half], pack[:, half:]], axis=0)


def call(body, out_shape, name, vmem, **options):
    return pl.pallas_call(
        body,
        out_shape=out_shape,
        name=name,
        compiler_params=pltpu.CompilerParams(vmem_limit_bytes=vmem * MIB),
        **options,
    )


def in_hbm(x):
    return pltpu.with_memory_space_constraint(x, pltpu.HBM)


def struct(shape, dtype=F32):
    return jax.ShapeDtypeStruct(shape, dtype)


VM = pl.BlockSpec(memory_space=pltpu.VMEM)
SM = pl.BlockSpec(memory_space=pltpu.SMEM)
HBM = pl.BlockSpec(memory_space=pltpu.HBM)


def climb_local(device, level, leaf_count, leaves, transfer_ref, gain_ref, local_ref):
    classes = level[0].shape[0]
    first, depth = 0, 0
    while len(level) > 1:
        count = len(level)
        gain_first = 2 * leaves - 2 * (leaves >> depth) + device * count
        scaled = []
        for i, weights in enumerate(level):
            local_ref[first + i] = weights
            scaled.append(weights * gain_ref[pl.ds(gain_first + i, 1), :])
        left = times(stacked(jnp.concatenate(scaled[0::2], axis=0)), *split(transfer_ref[depth, 0]))
        right = times(stacked(jnp.concatenate(scaled[1::2], axis=0)), *split(transfer_ref[depth, 1]))
        total = left + right
        first += count
        depth += 1
        level = [total[i * classes : (i + 1) * classes] for i in range(count // 2)]
    return level[0]


def leaf_weights(vector_ref, interp_ref, leaf_count, leaf_size, loads):
    found = []
    for j in range(leaf_count):
        if loads is not None:
            loads[j].wait()
        found.append(times(stacked(vector_ref[:, j * leaf_size : (j + 1) * leaf_size]), *split(interp_ref[j])))
    return found


def front(device, points, vector, leaf_skeleton, node_skeleton, leaf_interp, transfer, node_gain, leaves, reach):
    dim = points.shape[1]
    leaf_count, leaf_size, skel_size = leaf_interp.shape
    classes = vector.shape[0]
    pair_count = leaf_count - 1
    width = reach * leaf_size
    local_levels = leaf_count.bit_length() - 1

    def body(
        dev_ref, points_hbm, vector_hbm, leaf_ref, node_hbm, interp_hbm, transfer_hbm, gain_hbm,
        pack_ref, local_ref, hi_ref, lo_ref, head_ref, tail_ref,
        rows_ref, points_ref, vector_ref, interp_ref, transfer_ref, points_sem, vector_sem, interp_sem, transfer_sem,
        node_ref, gain_ref, node_sem, gain_sem,
    ):
        load_nodes = pltpu.make_async_copy(node_hbm, node_ref, node_sem)
        load_gains = pltpu.make_async_copy(gain_hbm, gain_ref, gain_sem)
        loads = [
            pltpu.make_async_copy(
                points_hbm.at[pl.ds(j * leaf_size, leaf_size)], points_ref.at[pl.ds(j * leaf_size, leaf_size)],
                points_sem.at[j],
            )
            for j in range(leaf_count)
        ]
        load_vector = pltpu.make_async_copy(vector_hbm, vector_ref, vector_sem)
        load_maps = pltpu.make_async_copy(transfer_hbm.at[pl.ds(0, local_levels)], transfer_ref, transfer_sem)
        interp_loads = [
            pltpu.make_async_copy(interp_hbm.at[j], interp_ref.at[j], interp_sem.at[j]) for j in range(leaf_count)
        ]
        for copy in [*loads, load_nodes, load_vector, *interp_loads, load_maps, load_gains]:
            copy.start()
        device = dev_ref[0]
        load_nodes.wait()
        rows_ref[...] = jnp.zeros_like(rows_ref)
        pair = 0
        for depth in range(1, local_levels + 1):
            count = leaf_count >> depth
            first = leaves - 2 * (leaves >> depth) + device * count
            for i in range(count):
                rows_ref[pair : pair + 1, :] = node_ref[pl.ds(first + i, 1), :]
                pair += 1
        leaf_columns, node_columns = columns(leaf_ref[...]), columns(rows_ref[...])
        level = []
        for j in range(leaf_count):
            loads[j].wait()
            cat = scaled_cat(points_ref[j * leaf_size : (j + 1) * leaf_size, :])
            level.append(nn(one_hot(leaf_columns[:, j : j + 1], leaf_size), cat).astype(BF16))
        pair = 0
        while len(level) > 1:
            above = []
            for p in range(len(level) // 2):
                left, right = level[2 * p], level[2 * p + 1]
                both = jnp.concatenate([left, right], axis=0)
                pick = one_hot(node_columns[:, pair : pair + 1], 2 * skel_size)
                above.append(nn(pick, both).astype(BF16))
                tile = pair_tile(left, right, half_norms(left)[0], half_norms(right)[1])
                hi_ref[pair], lo_ref[pair] = split(tile)
                pair += 1
            level = above
        whole = level[0]
        pack_skel(pack_ref, classes, whole[:, :dim].astype(F32) + whole[:, dim:].astype(F32))
        load_vector.wait()
        for ref, start in ((head_ref, 0), (tail_ref, (leaf_count - reach) * leaf_size)):
            ref[:width, :] = points_ref[start : start + width, :]
            for i in range(width // 128):
                ref[width + i * classes : width + (i + 1) * classes, :] = vector_ref[
                    :, start + i * 128 : start + (i + 1) * 128
                ]
        weights = leaf_weights(vector_ref, interp_ref, leaf_count, leaf_size, interp_loads)
        load_maps.wait()
        load_gains.wait()
        pack_ref[:classes] = climb_local(
            device, weights, leaf_count, leaves, transfer_ref, gain_ref, local_ref
        )

    return call(
        body,
        (
            struct((classes + skel_size // 2, skel_size)),
            struct((2 * leaf_count - 2, classes, skel_size)),
            struct((pair_count, skel_size, skel_size), BF16),
            struct((pair_count, skel_size, skel_size), BF16),
            struct((width + width // 128 * classes, 128)),
            struct((width + width // 128 * classes, 128)),
        ),
        "front",
        28,
        in_specs=[SM, HBM, HBM, VM, HBM, HBM, HBM, HBM],
        out_specs=(VM,) * 6,
        scratch_shapes=[
            pltpu.VMEM((leaf_count, skel_size), jnp.int32),
            pltpu.VMEM(points.shape, F32),
            pltpu.VMEM(vector.shape, F32),
            pltpu.VMEM(leaf_interp.shape, F32),
            pltpu.VMEM((local_levels,) + transfer.shape[1:], F32),
            pltpu.SemaphoreType.DMA((leaf_count,)),
            pltpu.SemaphoreType.DMA,
            pltpu.SemaphoreType.DMA((leaf_count,)),
            pltpu.SemaphoreType.DMA,
            pltpu.VMEM(node_skeleton.shape, jnp.int32),
            pltpu.VMEM(node_gain.shape, F32),
            pltpu.SemaphoreType.DMA,
            pltpu.SemaphoreType.DMA,
        ],
    )(
        device, in_hbm(points), in_hbm(vector), leaf_skeleton, in_hbm(node_skeleton), in_hbm(leaf_interp),
        in_hbm(transfer), in_hbm(node_gain),
    )


def upward(device, vector, gram, leaf_interp, transfer, node_gain, leaves):
    leaf_count, leaf_size, skel_size = leaf_interp.shape
    classes = vector.shape[0]
    local_levels = leaf_count.bit_length() - 1

    def body(dev_ref, vector_ref, gram_ref, interp_ref, transfer_ref, gain_ref, pack_ref, local_ref):
        weights = leaf_weights(vector_ref, interp_ref, leaf_count, leaf_size, None)
        pack_ref[:classes] = climb_local(
            dev_ref[0], weights, leaf_count, leaves, transfer_ref, gain_ref, local_ref
        )
        pack_ref[classes:] = gram_ref[...]

    return call(
        body,
        (
            struct((classes + gram.shape[0], skel_size)),
            struct((2 * leaf_count - 2, classes, skel_size)),
        ),
        "upward",
        18,
        in_specs=[SM, VM, VM, VM, VM, VM],
        out_specs=(VM, VM),
    )(device, vector, gram, leaf_interp, transfer, node_gain)


def apply_tile(mask, cat, hi, lo, out_ref, place):
    out_ref[place] = out_ref[place] + mask * times(cat, hi, lo)


def near_pairs(t, leaf_count):
    final = t == leaf_count - 2
    third = (jnp.where(final, t + 1, t), jnp.where(final, t + 1, t + 2), jnp.where(final, 0.0, 1.0))
    return [(t, t, None), (t, t + 1, 1.0), third]


def near_products(pairs, mask_ref, vecs, tile_ref, out_ref, reach):
    added = []
    for e, (a, b, both) in enumerate(pairs):
        mask = mask_ref[a, reach + b - a]
        hi, lo = tile_ref[0, e, 0], tile_ref[0, e, 1]
        added.append((b, mask * times(vecs[a], hi, lo)))
        if both is not None:
            added.append((a, (mask * both) * times(vecs[b], hi, lo, nt)))
    own = added[0][1] + added[2][1]
    out_ref[pairs[0][0]] = out_ref[pairs[0][0]] + own
    for place, value in [added[1], *added[3:]]:
        out_ref[place] = out_ref[place] + value


def near_build(points, vector, near_mask, base, first, count, leaf_count, reach):
    dim = points.shape[1]
    leaf_size = points.shape[0] // leaf_count
    classes = vector.shape[0]
    used = range(first, min(first + count + 2, leaf_count))

    def body(points_ref, vector_ref, mask_ref, *refs):
        base_ref = refs[0] if base is not None else None
        tile_ref, out_ref, cats, wides, rows, vecs = refs[-6:]

        @pl.when(pl.program_id(0) == 0)
        def _():
            out_ref[...] = jnp.zeros_like(out_ref) if base_ref is None else base_ref[...]
            for j in used:
                cat = scaled_cat(points_ref[j * leaf_size : (j + 1) * leaf_size, :])
                cats[j] = cat
                wide, row = half_norms(cat)
                wides[j] = wide
                rows[j] = jnp.broadcast_to(row, (8, leaf_size))
                vecs[j] = stacked(vector_ref[:, j * leaf_size : (j + 1) * leaf_size])

        pairs = near_pairs(pl.program_id(0) + first, leaf_count)
        for e, (a, b, _) in enumerate(pairs):
            tile = pair_tile(cats[a], cats[b], wides[a], rows[b][0:1, :])
            tile_ref[0, e, 0], tile_ref[0, e, 1] = split(tile)
        near_products(pairs, mask_ref, vecs, tile_ref, out_ref, reach)

    shape = (leaf_count, classes, leaf_size)
    whole = pl.BlockSpec(shape, lambda a: (0, 0, 0))
    return call(
        body,
        (pltpu.HBM((count, 3, 2, leaf_size, leaf_size), BF16), struct(shape)),
        "near_build",
        34,
        grid=(count,),
        in_specs=[
            pl.BlockSpec(points.shape, lambda a: (0, 0)),
            pl.BlockSpec(vector.shape, lambda a: (0, 0)),
            SM,
        ] + ([] if base is None else [whole]),
        out_specs=(pl.BlockSpec((1, 3, 2, leaf_size, leaf_size), lambda a: (a, 0, 0, 0, 0)), whole),
        scratch_shapes=[
            pltpu.VMEM((leaf_count, leaf_size, 2 * dim), BF16),
            pltpu.VMEM((leaf_count, leaf_size, 128), F32),
            pltpu.VMEM((leaf_count, 8, leaf_size), F32),
            pltpu.VMEM((leaf_count, 2 * classes, leaf_size), BF16),
        ],
    )(points, vector, near_mask, *([] if base is None else [base]))


def near_apply(tiles, vector, near_mask, base, first, leaf_count, reach):
    count, leaf_size = tiles.shape[0], tiles.shape[-1]
    classes = vector.shape[0]

    def body(tile_hbm, vector_ref, mask_ref, *refs):
        base_ref = refs[0] if base is not None else None
        out_ref, vecs, tile_ref, sems = refs[-4:]
        def loads(t):
            return [pltpu.make_async_copy(tile_hbm.at[t, e], tile_ref.at[t, e], sems.at[t, e]) for e in range(3)]

        for copy in loads(0):
            copy.start()
        out_ref[...] = jnp.zeros_like(out_ref) if base_ref is None else base_ref[...]
        for j in range(first, min(first + count + 2, leaf_count)):
            vecs[j] = stacked(vector_ref[:, j * leaf_size : (j + 1) * leaf_size])

        @pl.loop(0, count)
        def _(t):
            for copy in loads(t):
                copy.wait()

            @pl.when(t + 1 < count)
            def _():
                for copy in loads(t + 1):
                    copy.start()

            near_products(near_pairs(first + t, leaf_count), mask_ref, vecs, tile_ref.at[pl.ds(t, 1)], out_ref, reach)

    return call(
        body,
        struct((leaf_count, classes, leaf_size)),
        "near_apply",
        20,
        in_specs=[HBM, VM, SM] + ([] if base is None else [VM]),
        out_specs=VM,
        scratch_shapes=[
            pltpu.VMEM((leaf_count, 2 * classes, leaf_size), BF16),
            pltpu.VMEM(tiles.shape, BF16),
            pltpu.SemaphoreType.DMA((count, 3)),
        ],
    )(in_hbm(tiles), vector, near_mask, *([] if base is None else [base]))


def edges(leaf_count, reach):
    found = []
    for side in range(2):
        for h in range(reach):
            for j in range(reach):
                own = j if side == 0 else leaf_count - reach + j
                offset = h - reach - own if side == 0 else leaf_count + h - own
                if -reach <= offset <= reach:
                    found.append((side, h, j, own, reach + offset))
    return jnp.array(found, jnp.int32)


def edge_build(points, left, right, near_mask, classes, leaf_count, reach):
    dim = points.shape[1]
    leaf_size = points.shape[0] // leaf_count
    lanes = leaf_size // 128
    width = reach * leaf_size
    border = edges(leaf_count, reach)
    count = border.shape[0]

    def body(own_hbm, left_hbm, right_hbm, mask_ref, border_ref, tile_hbm, out_ref, tile_ref, halo_ref, own_ref, sems, out_sems):
        tail = pl.ds((leaf_count - reach) * leaf_size, width)
        loads = [
            pltpu.make_async_copy(src, dst, sems.at[i])
            for i, (src, dst) in enumerate(
                [
                    (left_hbm, halo_ref.at[0]), (right_hbm, halo_ref.at[1]),
                    (own_hbm.at[pl.ds(0, width)], own_ref.at[0]), (own_hbm.at[tail], own_ref.at[1]),
                ]
            )
        ]
        for copy in loads:
            copy.start()
        out_ref[...] = jnp.zeros_like(out_ref)
        for copy in loads:
            copy.wait()

        def cat_of(ref, i, spot):
            return scaled_cat(ref[i, pl.ds(pl.multiple_of(spot * leaf_size, leaf_size), leaf_size), :])

        def rows_of(i, spot):
            firsts = [pl.multiple_of(width + (spot * lanes + n) * classes, classes) for n in range(lanes)]
            return jnp.concatenate([halo_ref[i, pl.ds(f, classes), :] for f in firsts], axis=1)

        def store(t):
            return pltpu.make_async_copy(tile_ref.at[t], tile_hbm.at[t], out_sems.at[t])

        @pl.loop(0, count)
        def _(t):
            side, h, j, own, slot = [border_ref[t, i] for i in range(5)]
            cat_h, cat_j = cat_of(halo_ref, side, h), cat_of(own_ref, side, j)
            tile = pair_tile(cat_h, cat_j, half_norms(cat_h)[0], half_norms(cat_j)[1])
            tile_ref[t, 0], tile_ref[t, 1] = split(tile)
            store(t).start()
            apply_tile(
                mask_ref[own, slot], stacked(rows_of(side, h)), tile_ref[t, 0], tile_ref[t, 1], out_ref,
                side * reach + j,
            )

        @pl.loop(0, count)
        def _(t):
            store(t).wait()

    shape = (count, 2, leaf_size, leaf_size)
    return call(
        body,
        (pltpu.HBM(shape, BF16), struct((2 * reach, classes, leaf_size))),
        "edge_build",
        22,
        in_specs=[HBM, HBM, HBM, SM, SM],
        out_specs=(HBM, VM),
        scratch_shapes=[
            pltpu.VMEM(shape, BF16),
            pltpu.VMEM((2,) + left.shape, F32),
            pltpu.VMEM((2, width, dim), F32),
            pltpu.SemaphoreType.DMA((4,)),
            pltpu.SemaphoreType.DMA((count,)),
        ],
    )(in_hbm(points), in_hbm(left), in_hbm(right), near_mask, border)


def edge_apply(tiles, left_rows, right_rows, near_mask, leaf_count, reach):
    count, leaf_size = tiles.shape[0], tiles.shape[-1]
    classes = left_rows.shape[0]

    def body(tile_hbm, lv_ref, rv_ref, mask_ref, border_ref, out_ref, tile_ref, vecs, sems):
        def load(t):
            return pltpu.make_async_copy(tile_hbm.at[t], tile_ref.at[t], sems.at[t])

        for t in range(min(3, count)):
            load(t).start()
        out_ref[...] = jnp.zeros_like(out_ref)
        for h in range(reach):
            where = slice(h * leaf_size, (h + 1) * leaf_size)
            vecs[0, h] = stacked(lv_ref[:, where])
            vecs[1, h] = stacked(rv_ref[:, where])

        @pl.loop(0, count)
        def _(t):
            side, h, j, own, slot = [border_ref[t, i] for i in range(5)]
            load(t).wait()

            @pl.when(t + 3 < count)
            def _():
                load(t + 3).start()

            apply_tile(
                mask_ref[own, slot], vecs[side, h], tile_ref[t, 0], tile_ref[t, 1], out_ref, side * reach + j
            )

    return call(
        body,
        struct((2 * reach, classes, leaf_size)),
        "edge_apply",
        14,
        in_specs=[HBM, VM, VM, SM, SM],
        out_specs=VM,
        scratch_shapes=[
            pltpu.VMEM(tiles.shape, BF16),
            pltpu.VMEM((2, reach, 2 * classes, leaf_size), BF16),
            pltpu.SemaphoreType.DMA((count,)),
        ],
    )(in_hbm(tiles), left_rows, right_rows, near_mask, edges(leaf_count, reach))


def tree_stage(device, packs, node_gain, transfer, node_skeleton, classes, leaves, level, bit, with_skel, extra, climb):
    count = len(packs)
    skel_size = packs[0].shape[1]
    levels = count.bit_length() - 1
    skel_rows = skel_size // 2 if with_skel else 0
    out_rows = packs[0].shape[0]

    def body(*refs):
        dev_ref, pack_refs = refs[0], refs[1 : 1 + count]
        rest = list(refs[1 + count :])
        gains_ref, transfer_ref = rest.pop(0), rest.pop(0)
        node_ref = rest.pop(0) if with_skel else None
        sibling_ref = rest.pop(0)
        next_ref = rest.pop(0)
        hi_ref, lo_ref = (rest.pop(0), rest.pop(0)) if with_skel else (None, None)
        joined = rest.pop(0)
        device = dev_ref[0]
        place = lax.shift_right_logical(device, bit) & (count - 1)
        base = lax.shift_right_logical(device, bit + levels)
        if with_skel and (climb or levels > 1):
            rows_ref = rest.pop(0)
            rows_ref[...] = jnp.zeros_like(rows_ref)
            spot = 0
            for depth in range(1, levels + 1 if climb else levels):
                nodes = count >> depth
                row = leaves - 2 * (leaves >> (level + depth)) + base * nodes
                for i in range(nodes):
                    rows_ref[spot : spot + 1, :] = node_ref[pl.ds(row + i, 1), :]
                    spot += 1
            pick_columns = columns(rows_ref[...])
        for i in range(count):
            joined[place ^ i] = pack_refs[i][...]
        weights = [joined[i][:classes] for i in range(count)]
        skels = []
        if with_skel:
            skels = [
                jnp.concatenate(split(unpack_skel(joined[i][classes : classes + skel_rows])), axis=1)
                for i in range(count)
            ]
        pick_first = 0
        for depth in range(levels):
            own = lax.shift_right_logical(place, depth)
            other = own ^ 1
            chosen = weights[0]
            for i in range(1, len(weights)):
                chosen = jnp.where(other == i, weights[i], chosen)
            sibling_ref[depth] = chosen
            if with_skel:
                mine, theirs = skels[0], skels[0]
                for i in range(1, len(skels)):
                    mine = jnp.where(own == i, skels[i], mine)
                    theirs = jnp.where(other == i, skels[i], theirs)
                tile = pair_tile(theirs, mine, half_norms(theirs)[0], half_norms(mine)[1])
                hi_ref[depth], lo_ref[depth] = split(tile)
            if depth + 1 < levels or climb:
                row = 2 * leaves - 2 * (leaves >> (level + depth)) + base * len(weights)
                scaled = [w * gains_ref[pl.ds(row + i, 1), :] for i, w in enumerate(weights)]
                left = times(stacked(jnp.concatenate(scaled[0::2], axis=0)), *split(transfer_ref[depth, 0]))
                right = times(stacked(jnp.concatenate(scaled[1::2], axis=0)), *split(transfer_ref[depth, 1]))
                total = left + right
                weights = [total[i * classes : (i + 1) * classes] for i in range(len(weights) // 2)]
                if with_skel:
                    above = []
                    for p in range(len(skels) // 2):
                        both = jnp.concatenate([skels[2 * p], skels[2 * p + 1]], axis=0)
                        pick = one_hot(pick_columns[:, pick_first : pick_first + 1], 2 * skel_size)
                        above.append(nn(pick, both).astype(BF16))
                        pick_first += 1
                    skels = above
        if climb:
            next_ref[:classes] = weights[0]
            if with_skel:
                dim = skels[0].shape[1] // 2
                pack_skel(next_ref, classes, skels[0][:, :dim].astype(F32) + skels[0][:, dim:].astype(F32))
        else:
            next_ref[: classes + skel_rows] = jnp.zeros((classes + skel_rows, skel_size), F32)
        if extra:
            rows = slice(classes + skel_rows, out_rows)
            total = joined[0][rows]
            for i in range(1, count):
                total = total + joined[i][rows]
            next_ref[rows] = total

    out = [struct((levels, classes, skel_size)), struct((out_rows, skel_size))]
    if with_skel:
        out += [struct((levels, skel_size, skel_size), BF16)] * 2
    scratch = [pltpu.VMEM((count, out_rows, skel_size), F32)]
    ins = [device, *packs, node_gain, transfer]
    if with_skel:
        ins.append(node_skeleton)
        if climb or levels > 1:
            scratch.append(pltpu.VMEM((8, skel_size), jnp.int32))
    return call(
        body,
        tuple(out),
        "tree_stage",
        10,
        in_specs=[SM] + [VM] * (len(ins) - 1),
        out_specs=tuple([VM] * len(out)),
        scratch_shapes=scratch,
    )(*ins)


def downward(
    device, vector, near, edge, leaf_interp, transfer, local_weights, local_tiles, node_gain,
    siblings, device_tiles, reach, leaves, start,
):
    leaf_count, leaf_size, skel_size = leaf_interp.shape
    classes = vector.shape[0]
    local_levels = leaf_count.bit_length() - 1
    stages = len(siblings)

    def body(*refs):
        dev_ref, vector_ref, near_ref, edge_ref, interp_ref, maps_ref = refs[:6]
        weights_ref, tiles_hi, tiles_lo, gain_ref = refs[6:10]
        sib_refs = refs[10 : 10 + stages]
        dev_refs = refs[10 + stages : 10 + 3 * stages]
        rest = list(refs[10 + 3 * stages :])
        device = dev_ref[0]

        def gain(level, node):
            return gain_ref[pl.ds(2 * leaves - 2 * (leaves >> level) + node, 1), :]

        image_ref = rest.pop(0)
        head_ref, tail_ref = (rest.pop(0), rest.pop(0)) if start else (None, None)
        gram_ref = rest.pop(0) if start else None
        local = []
        for s in range(stages):
            for i in range(sib_refs[s].shape[0]):
                local.append(times(stacked(sib_refs[s][i]), dev_refs[2 * s][i], dev_refs[2 * s + 1][i]))
        top = len(local) - 1
        potential = local[top]
        for b in range(top - 1, -1, -1):
            node = lax.shift_right_logical(device, b)
            down = maps_ref[local_levels + b, node & 1]
            potential = times(stacked(potential), *split(down), nt) * gain(local_levels + b, node) + local[b]
        level = [potential]
        for depth in range(local_levels - 1, -1, -1):
            cat = stacked(jnp.concatenate(level, axis=0))
            sides = [times(cat, *split(maps_ref[depth, c]), nt) for c in range(2)]
            count = leaf_count >> depth
            first = 2 * leaf_count - 2 * count
            pair_first = leaf_count - count
            below = []
            for n in range(count):
                p, c = n // 2, n % 2
                cat_sibling = stacked(weights_ref[first + (n ^ 1)])
                hi, lo = tiles_hi[pair_first + p], tiles_lo[pair_first + p]
                direct = times(cat_sibling, hi, lo, nn if c else nt)
                carried = sides[c][p * classes : (p + 1) * classes]
                below.append(carried * gain(depth, device * count + n) + direct)
            level = below
        for j in range(leaf_count):
            where = slice(j * leaf_size, (j + 1) * leaf_size)
            total = ridge * vector_ref[:, where] + near_ref[j]
            if j < reach:
                total = total + edge_ref[j]
            if j >= leaf_count - reach:
                total = total + edge_ref[reach + j - (leaf_count - reach)]
            image_ref[:, where] = total + times(stacked(level[j]), *split(interp_ref[j]), nt)
        if start:
            width = reach * leaf_size
            head_ref[...] = image_ref[:, :width]
            tail_ref[...] = image_ref[:, (leaf_count - reach) * leaf_size :]
            whole = nt(stacked(vector_ref[...]), jnp.concatenate([stacked(vector_ref[...]), stacked(image_ref[...])], axis=0))
            half = whole[:classes] + whole[classes:]
            rows = classes // 2
            self_gram = half[:, :classes] + half[:, classes : 2 * classes]
            image_gram = half[:, 2 * classes : 3 * classes] + half[:, 3 * classes :]
            gram = jnp.concatenate([self_gram, image_gram], axis=1)
            gram_ref[:, : 2 * classes] = gram[:rows]
            gram_ref[:, 2 * classes :] = gram[rows:]

    out = [struct(vector.shape)]
    if start:
        out += [struct((classes, reach * leaf_size))] * 2
        out.append(struct((classes // 2, 4 * classes)))
    ins = [device, vector, near, edge, leaf_interp, transfer, local_weights, *local_tiles, node_gain]
    ins += list(siblings)
    for pair in device_tiles:
        ins += list(pair)
    specs = [SM] + [VM] * (len(ins) - 1)
    return call(
        body,
        tuple(out),
        "downward",
        30,
        in_specs=specs,
        out_specs=tuple([VM] * len(out)),
    )(*ins)


def mixed(matrix, rows):
    m_hi, m_lo = split(matrix)
    r_hi, r_lo = split(rows)
    return nn(
        jnp.concatenate([m_hi, m_lo, m_hi, m_lo], axis=1),
        jnp.concatenate([r_hi, r_hi, r_lo, r_lo], axis=0),
    )


def three(x):
    hi = x.astype(BF16)
    rest = x - hi.astype(F32)
    mid = rest.astype(BF16)
    return hi, mid, (rest - mid.astype(F32)).astype(BF16)


def exact_dot(a, b):
    a0, a1, a2 = three(a)
    b0, b1, b2 = three(b)
    return nn(
        jnp.concatenate([a2, a1, a0, a1, a0, a0], axis=1),
        jnp.concatenate([b0, b1, b2, b0, b1, b0], axis=0),
    )


def eliminate(systems, width=4):
    size, wide = systems[0].shape
    place = lax.broadcasted_iota(jnp.int32, (size, wide), 0)
    for first in range(0, size, width):
        block = [
            [jnp.broadcast_to(m[:, k : k + 1], (size, wide)) for k in range(first, first + width)]
            for m in systems
        ]
        for i in range(width):
            k = first + i
            pivot = place == k
            for n in range(len(systems)):
                cols = block[n]
                inverse = 1.0 / cols[i][k : k + 1, :]
                for j in range(i + 1, width):
                    scaled = cols[j][k : k + 1, :] * inverse
                    cols[j] = jnp.where(pivot, scaled, cols[j] - cols[i] * scaled)
                scaled = systems[n][k : k + 1, :] * inverse
                systems[n] = jnp.where(pivot, scaled, systems[n] - cols[i] * scaled)
    return systems


def first_step(gram, right_side, image, second):
    classes = right_side.shape[0]

    def body(gram_in, b_ref, image_ref, second_ref, res_ref, res_image_ref, gram_ref, small_ref):
        packed = gram_in[classes:, :]
        both = jnp.concatenate([packed[:, : 2 * classes], packed[:, 2 * classes :]], axis=0)
        turned = both.T
        base = 0.5 * (both[:, :classes] + turned[:classes])
        curvature = 0.5 * (both[:, classes:] + turned[classes:])
        square = (classes, classes)
        unit = jnp.where(
            lax.broadcasted_iota(jnp.int32, square, 0) == lax.broadcasted_iota(jnp.int32, square, 1), 1.0, 0.0
        )
        solved, inverse = eliminate(
            [jnp.concatenate([curvature, base], axis=1), jnp.concatenate([base, unit], axis=1)]
        )
        alpha_t = solved.T[classes:]
        small_ref[:classes] = jnp.concatenate([alpha_t, inverse[:, classes:]], axis=1)
        small_ref[classes:] = both
        res = b_ref[...] - mixed(alpha_t, image_ref[...])
        res_image = image_ref[...] - mixed(alpha_t, second_ref[...])
        res_ref[...] = res
        res_image_ref[...] = res_image
        res_cat, base_cat = stacked(res), stacked(b_ref[...])
        left = jnp.concatenate([res_cat, base_cat], axis=0)
        right = jnp.concatenate([res_cat, stacked(res_image), stacked(image_ref[...])], axis=0)
        whole = nt(left, right)

        def block(i, j):
            part = whole[2 * i * classes : 2 * (i + 1) * classes, 2 * j * classes : 2 * (j + 1) * classes]
            half = part[:classes] + part[classes:]
            return half[:, :classes] + half[:, classes:]

        gram_ref[...] = jnp.concatenate([block(0, 0), block(0, 1), block(0, 2), block(1, 1)], axis=1)

    return call(
        body,
        (
            struct(right_side.shape),
            struct(right_side.shape),
            struct((classes, 4 * classes)),
            struct((2 * classes, 2 * classes)),
        ),
        "first_step",
        28,
    )(gram, right_side, image, second)


def last_step(small, parts, right_side, image, res, res_image):
    classes = right_side.shape[0]
    count = len(parts)

    def body(small_ref, *refs):
        base_ref, image_ref, res_ref, res_image_ref, sol_ref, out_ref = refs[count:]
        grams = [ref[...] for ref in refs[:count]]
        while len(grams) > 1:
            grams = [a + b for a, b in zip(grams[0::2], grams[1::2])]
        grams = grams[0]
        alpha_t = small_ref[:classes, :classes]
        inverse = small_ref[:classes, classes:]
        image_gram = small_ref[classes:, classes:]
        new_gram = grams[:, :classes]
        new_gram = 0.5 * (new_gram + grams[:, : 2 * classes].T[:classes])
        beta = exact_dot(inverse, new_gram)
        beta_t = jnp.concatenate([beta, beta], axis=1).T[:classes]
        res_image_gram = grams[:, classes : 2 * classes]
        res_base = grams[:, 2 * classes : 3 * classes]
        base_res = grams[:, 3 * classes :]
        curvature = (
            res_image_gram
            + exact_dot(res_base, beta)
            + exact_dot(beta_t, base_res + exact_dot(image_gram, beta))
        )
        curvature = 0.5 * (curvature + jnp.concatenate([curvature, curvature], axis=1).T[:classes])
        (solved,) = eliminate([jnp.concatenate([curvature, new_gram], axis=1)])
        alpha2_t = solved.T[classes:]
        direction = res_ref[...] + mixed(beta_t, base_ref[...])
        moved = res_image_ref[...] + mixed(beta_t, image_ref[...])
        sol_ref[...] = mixed(alpha_t, base_ref[...]) + mixed(alpha2_t, direction)
        out_ref[...] = res_ref[...] - mixed(alpha2_t, moved)

    return call(body, (struct(right_side.shape), struct(right_side.shape)), "last_step", 28)(
        small, *parts, right_side, image, res, res_image
    )


def body(
    points, right_side, neighbours, leaf_interp, leaf_skeleton, node_skeleton, node_gain, transfer
):
    leaf_count, slot_count = neighbours.shape
    reach = (slot_count - 1) // 2
    leaf_size, skel_size = leaf_interp.shape[1:]
    classes = right_side.shape[0]
    dev_count = lax.axis_size("leaf")
    dev_levels = dev_count.bit_length() - 1
    local_levels = leaf_count.bit_length() - 1
    levels = local_levels + dev_levels
    leaves = leaf_count * dev_count
    device = lax.axis_index("leaf").astype(jnp.int32)[None]

    def exchange(head, tail):
        ends = dev_count - 1
        left = lax.ppermute(tail, "leaf", [(i, i + 1) for i in range(ends)])
        right = lax.ppermute(head, "leaf", [(i + 1, i) for i in range(ends)])
        return left, right

    def group(pack, first_bit, count):
        return [pack] + [
            lax.ppermute(pack, "leaf", [(d, d ^ (i << first_bit)) for d in range(dev_count)])
            for i in range(1, count)
        ]

    stages = [(bit, min(2, dev_levels - bit)) for bit in range(0, dev_levels, 2)]
    near_mask = (neighbours >= 0).astype(F32)

    def climb(pack, with_skel, extra, covers):
        siblings, tiles, results = [], [], []
        for stage, (bit, width) in enumerate(stages):
            level = local_levels + bit
            depth = min(width, levels - 1 - level) or 1
            first = min(level, levels - 1 - depth)
            packs = group(pack, bit, 1 << width)
            if stage < len(covers):
                done = covers[stage](pack)
                results.append(done)
                packs, _ = lax.optimization_barrier((packs, done[-1]))
            found = tree_stage(
                device, packs, node_gain, lax.slice_in_dim(transfer, first, first + depth, axis=0),
                node_skeleton, classes, leaves, level, bit, with_skel, extra, level + width < levels,
            )
            siblings.append(found[0])
            pack = found[1]
            if with_skel:
                tiles.append((found[2], found[3]))
        return siblings, tiles, pack, results

    def after(pack, *values):
        return lax.optimization_barrier((pack, values))[1]

    assert reach == 2
    steps = leaf_count - 1
    cuts = [0, -(-steps * 3 // 7), -(-steps * 5 // 7), steps]

    pack, weights, *local_tiles, head, tail = front(
        device, points, right_side, leaf_skeleton, node_skeleton, leaf_interp, transfer, node_gain, leaves, reach
    )
    left, right = exchange(head, tail)
    near_tiles, total = [], [None]

    def build(part):
        def run(pack):
            (vector,) = after(pack, right_side)
            tiles, total[0] = near_build(
                points, vector, near_mask, total[0], cuts[part], cuts[part + 1] - cuts[part], leaf_count, reach
            )
            near_tiles.append(tiles)
            return total[0],

        return run

    def build_last(pack):
        build(2)(pack)
        left_pack, right_pack, _ = after(pack, left, right, total[0])
        return edge_build(points, left_pack, right_pack, near_mask, classes, leaf_count, reach)

    siblings, device_tiles, _, results = climb(pack, True, False, [build(0), build(1), build_last])
    near = total[0]
    edge_tiles, edge = results[2]
    image, head, tail, gram = downward(
        device, right_side, near, edge, leaf_interp, transfer, weights, local_tiles, node_gain,
        siblings, device_tiles, reach, leaves, True,
    )

    pack, weights = upward(device, image, gram, leaf_interp, transfer, node_gain, leaves)
    left_rows, right_rows = exchange(*after(pack, head, tail))
    total = [None]

    def apply(part):
        def run(pack):
            (vector,) = after(pack, image)
            total[0] = near_apply(near_tiles[part], vector, near_mask, total[0], cuts[part], leaf_count, reach)
            return total[0],

        return run

    def apply_last(pack):
        apply(2)(pack)
        left, right, _ = after(pack, left_rows, right_rows, total[0])
        return (edge_apply(edge_tiles, left, right, near_mask, leaf_count, reach),)

    siblings, _, pack, results = climb(pack, False, True, [apply(0), apply(1), apply_last])
    near, (edge,) = total[0], results[2]
    (second,) = downward(
        device, image, near, edge, leaf_interp, transfer, weights, local_tiles, node_gain,
        siblings, device_tiles, reach, leaves, False,
    )

    res, res_image, grams, small = first_step(pack, right_side, image, second)
    for bit, width in stages[:-1]:
        parts = group(grams, bit, 1 << width)
        while len(parts) > 1:
            parts = [a + b for a, b in zip(parts[0::2], parts[1::2])]
        grams = parts[0]
    bit, width = stages[-1]
    parts = group(grams, bit, 1 << width)
    return last_step(small, parts, right_side, image, res, res_image)


def solution(mesh):
    placed = (
        P("leaf", None),
        P(None, "leaf"),
        P("leaf", None),
        P("leaf", None, None),
        P("leaf", None),
        P(),
        P(),
        P(),
    )
    return jax.shard_map(
        body,
        mesh=mesh,
        in_specs=placed,
        out_specs=(P(None, "leaf"), P(None, "leaf")),
        check_vma=False,
    )
```

```python
import math

import jax
import jax.numpy as jnp
from jax import lax
from jax.experimental import pallas as pl
from jax.experimental.pallas import tpu as pltpu
from jax.sharding import PartitionSpec as P

ITERS = 2
ridge = 1.0
F32 = jnp.float32
BF16 = jnp.bfloat16
COORD_SCALE = math.sqrt(math.log2(math.e))
MIB = 1024 * 1024


def nn(a, b):
    return lax.dot_general(a, b, (((1,), (0,)), ((), ())), preferred_element_type=F32)


def nt(a, b):
    return lax.dot_general(a, b, (((1,), (1,)), ((), ())), preferred_element_type=F32)


def split(x):
    hi = x.astype(BF16)
    return hi, (x - hi.astype(F32)).astype(BF16)


def stacked(x):
    return jnp.concatenate(split(x), axis=0)


def times(cat, b_hi, b_lo, mul=nn):
    rows = cat.shape[0] // 2
    both = mul(cat, b_hi)
    return both[:rows] + both[rows:] + mul(cat[:rows], b_lo)


def scaled_cat(x):
    return jnp.concatenate(split(x * COORD_SCALE), axis=1)


def half_norms(cat):
    dim = cat.shape[1] // 2
    whole = cat[:, :dim].astype(F32) + cat[:, dim:].astype(F32)
    column = 0.5 * jnp.sum(whole * whole, axis=1, keepdims=True)
    wide = jnp.broadcast_to(column, (column.shape[0], 128))
    return wide, wide.T[0:1, :]


def pair_tile(cat_a, cat_b, wide_a, row_b):
    dim = cat_b.shape[1] // 2
    b_hi, b_lo = cat_b[:, :dim], cat_b[:, dim:]
    inner = nt(
        jnp.concatenate([cat_a, cat_a], axis=1),
        jnp.concatenate([b_hi, b_hi, b_lo, b_lo], axis=1),
    )
    count = cat_b.shape[0] // 128
    return jnp.exp2(inner - jnp.concatenate([wide_a] * count, axis=1) - row_b)


def one_hot(column, width):
    rows = column.shape[0]
    spots = lax.broadcasted_iota(jnp.int32, (rows, width), 1).astype(F32)
    return jnp.where(spots == column, 1.0, 0.0).astype(BF16)


def columns(rows):
    return rows.astype(F32).T


def pack_skel(ref, first, skel):
    half = skel.shape[0] // 2
    ref[first : first + half, : skel.shape[1]] = skel[:half]
    ref[first : first + half, skel.shape[1] :] = skel[half:]


def unpack_skel(pack):
    half = pack.shape[1] // 2
    return jnp.concatenate([pack[:, :half], pack[:, half:]], axis=0)


def call(body, out_shape, name, vmem, **options):
    return pl.pallas_call(
        body,
        out_shape=out_shape,
        name=name,
        compiler_params=pltpu.CompilerParams(vmem_limit_bytes=vmem * MIB),
        **options,
    )


def in_hbm(x):
    return pltpu.with_memory_space_constraint(x, pltpu.HBM)


def struct(shape, dtype=F32):
    return jax.ShapeDtypeStruct(shape, dtype)


VM = pl.BlockSpec(memory_space=pltpu.VMEM)
SM = pl.BlockSpec(memory_space=pltpu.SMEM)
HBM = pl.BlockSpec(memory_space=pltpu.HBM)


def climb_local(device, level, leaf_count, leaves, transfer_ref, gain_ref, local_ref):
    classes = level[0].shape[0]
    first, depth = 0, 0
    while len(level) > 1:
        count = len(level)
        gain_first = 2 * leaves - 2 * (leaves >> depth) + device * count
        scaled = []
        for i, weights in enumerate(level):
            local_ref[first + i] = weights
            scaled.append(weights * gain_ref[pl.ds(gain_first + i, 1), :])
        left = times(stacked(jnp.concatenate(scaled[0::2], axis=0)), *split(transfer_ref[depth, 0]))
        right = times(stacked(jnp.concatenate(scaled[1::2], axis=0)), *split(transfer_ref[depth, 1]))
        total = left + right
        first += count
        depth += 1
        level = [total[i * classes : (i + 1) * classes] for i in range(count // 2)]
    return level[0]


def leaf_weights(vector_ref, interp_ref, leaf_count, leaf_size):
    found = []
    for j in range(leaf_count):
        found.append(times(stacked(vector_ref[:, j * leaf_size : (j + 1) * leaf_size]), *split(interp_ref[j])))
    return found


def front(device, points, vector, leaf_skeleton, node_skeleton, leaf_count, leaves, reach):
    dim = points.shape[1]
    leaf_size, skel_size = points.shape[0] // leaf_count, leaf_skeleton.shape[1]
    classes = vector.shape[0]
    pair_count = leaf_count - 1
    width = reach * leaf_size
    local_levels = leaf_count.bit_length() - 1

    def body(
        dev_ref, points_hbm, vector_hbm, leaf_ref, node_hbm,
        pack_ref, hi_ref, lo_ref, head_ref, tail_ref,
        rows_ref, points_ref, ends_ref, node_ref, points_sem, ends_sem, node_sem,
    ):
        load_nodes = pltpu.make_async_copy(node_hbm, node_ref, node_sem)
        loads = [
            pltpu.make_async_copy(
                points_hbm.at[pl.ds(j * leaf_size, leaf_size)], points_ref.at[pl.ds(j * leaf_size, leaf_size)],
                points_sem.at[j],
            )
            for j in range(leaf_count)
        ]
        starts = (0, (leaf_count - reach) * leaf_size)
        end_loads = [
            pltpu.make_async_copy(vector_hbm.at[:, pl.ds(starts[i], width)], ends_ref.at[i], ends_sem.at[i])
            for i in range(2)
        ]
        for copy in [load_nodes, *loads, *end_loads]:
            copy.start()
        device = dev_ref[0]
        rows_ref[...] = jnp.zeros_like(rows_ref)
        load_nodes.wait()
        pair = 0
        for depth in range(1, local_levels + 1):
            count = leaf_count >> depth
            first = leaves - 2 * (leaves >> depth) + device * count
            for i in range(count):
                rows_ref[pair : pair + 1, :] = node_ref[pl.ds(first + i, 1), :]
                pair += 1
        leaf_columns, node_columns = columns(leaf_ref[...]), columns(rows_ref[...])
        level = []
        for j in range(leaf_count):
            loads[j].wait()
            cat = scaled_cat(points_ref[j * leaf_size : (j + 1) * leaf_size, :])
            level.append(nn(one_hot(leaf_columns[:, j : j + 1], leaf_size), cat).astype(BF16))
        for i, ref in enumerate((head_ref, tail_ref)):
            end_loads[i].wait()
            ref[:width, :] = points_ref[starts[i] : starts[i] + width, :]
            for n in range(width // 128):
                ref[width + n * classes : width + (n + 1) * classes, :] = ends_ref[i, :, n * 128 : (n + 1) * 128]
        pair = 0
        while len(level) > 1:
            above = []
            for p in range(len(level) // 2):
                left, right = level[2 * p], level[2 * p + 1]
                both = jnp.concatenate([left, right], axis=0)
                pick = one_hot(node_columns[:, pair : pair + 1], 2 * skel_size)
                above.append(nn(pick, both).astype(BF16))
                tile = pair_tile(left, right, half_norms(left)[0], half_norms(right)[1])
                hi_ref[pair], lo_ref[pair] = split(tile)
                pair += 1
            level = above
        whole = level[0]
        pack_skel(pack_ref, 0, whole[:, :dim].astype(F32) + whole[:, dim:].astype(F32))

    return call(
        body,
        (
            struct((skel_size // 2, skel_size)),
            struct((pair_count, skel_size, skel_size), BF16),
            struct((pair_count, skel_size, skel_size), BF16),
            struct((width + width // 128 * classes, 128)),
            struct((width + width // 128 * classes, 128)),
        ),
        "front",
        20,
        in_specs=[SM, HBM, HBM, VM, HBM],
        out_specs=(VM,) * 5,
        scratch_shapes=[
            pltpu.VMEM((leaf_count, skel_size), jnp.int32),
            pltpu.VMEM(points.shape, F32),
            pltpu.VMEM((2, classes, width), F32),
            pltpu.VMEM(node_skeleton.shape, jnp.int32),
            pltpu.SemaphoreType.DMA((leaf_count,)),
            pltpu.SemaphoreType.DMA((2,)),
            pltpu.SemaphoreType.DMA,
        ],
    )(device, in_hbm(points), in_hbm(vector), leaf_skeleton, in_hbm(node_skeleton))


def upward(device, vector, gram, leaf_interp, transfer, node_gain, leaves):
    leaf_count, leaf_size, skel_size = leaf_interp.shape
    classes = vector.shape[0]
    local_levels = leaf_count.bit_length() - 1

    def body(dev_ref, vector_ref, gram_ref, interp_ref, transfer_ref, gain_ref, pack_ref, local_ref):
        weights = leaf_weights(vector_ref, interp_ref, leaf_count, leaf_size)
        pack_ref[:classes] = climb_local(
            dev_ref[0], weights, leaf_count, leaves, transfer_ref, gain_ref, local_ref
        )
        pack_ref[classes:] = gram_ref[...]

    return call(
        body,
        (
            struct((classes + gram.shape[0], skel_size)),
            struct((2 * leaf_count - 2, classes, skel_size)),
        ),
        "upward",
        18,
        in_specs=[SM, VM, VM, VM, VM, VM],
        out_specs=(VM, VM),
    )(device, vector, gram, leaf_interp, transfer, node_gain)


def apply_tile(neighbour, cat, hi, lo, out_ref, place):
    mask = jnp.where(neighbour >= 0, 1.0, 0.0)
    out_ref[place] = out_ref[place] + mask * times(cat, hi, lo)


def near_pairs(t, leaf_count):
    final = t == leaf_count - 2
    third = (jnp.where(final, t + 1, t), jnp.where(final, t + 1, t + 2), jnp.where(final, 0.0, 1.0))
    return [(t, t, None), (t, t + 1, 1.0), third]


def near_products(pairs, mask_ref, vecs, tile_ref, out_ref, reach):
    added = []
    for e, (a, b, both) in enumerate(pairs):
        mask = jnp.where(mask_ref[a, reach + b - a] >= 0, 1.0, 0.0)
        hi, lo = tile_ref[0, e, 0], tile_ref[0, e, 1]
        added.append((b, mask * times(vecs[a], hi, lo)))
        if both is not None:
            added.append((a, (mask * both) * times(vecs[b], hi, lo, nt)))
    own = added[0][1] + added[2][1]
    out_ref[pairs[0][0]] = out_ref[pairs[0][0]] + own
    for place, value in [added[1], *added[3:]]:
        out_ref[place] = out_ref[place] + value


def near_build(points, vector, near_mask, base, first, count, leaf_count, reach):
    dim = points.shape[1]
    leaf_size = points.shape[0] // leaf_count
    classes = vector.shape[0]
    used = range(first, min(first + count + 2, leaf_count))

    def body(points_ref, vector_ref, mask_ref, *refs):
        base_ref = refs[0] if base is not None else None
        tile_ref, out_ref, cats, wides, rows, vecs = refs[-6:]

        @pl.when(pl.program_id(0) == 0)
        def _():
            out_ref[...] = jnp.zeros_like(out_ref) if base_ref is None else base_ref[...]

            @pl.loop(used[0], used[-1] + 1)
            def _(j):
                where = pl.ds(pl.multiple_of(j * leaf_size, leaf_size), leaf_size)
                cat = scaled_cat(points_ref[where, :])
                cats[j] = cat
                wide, row = half_norms(cat)
                wides[j] = wide
                rows[j] = jnp.broadcast_to(row, (8, leaf_size))
                vecs[j] = stacked(vector_ref[:, where])

        pairs = near_pairs(pl.program_id(0) + first, leaf_count)
        for e, (a, b, _) in enumerate(pairs):
            tile = pair_tile(cats[a], cats[b], wides[a], rows[b][0:1, :])
            tile_ref[0, e, 0], tile_ref[0, e, 1] = split(tile)
        near_products(pairs, mask_ref, vecs, tile_ref, out_ref, reach)

    shape = (leaf_count, classes, leaf_size)
    whole = pl.BlockSpec(shape, lambda a: (0, 0, 0))
    return call(
        body,
        (pltpu.HBM((count, 3, 2, leaf_size, leaf_size), BF16), struct(shape)),
        "near_build",
        34,
        grid=(count,),
        in_specs=[
            pl.BlockSpec(points.shape, lambda a: (0, 0)),
            pl.BlockSpec(vector.shape, lambda a: (0, 0)),
            SM,
        ] + ([] if base is None else [whole]),
        out_specs=(pl.BlockSpec((1, 3, 2, leaf_size, leaf_size), lambda a: (a, 0, 0, 0, 0)), whole),
        scratch_shapes=[
            pltpu.VMEM((leaf_count, leaf_size, 2 * dim), BF16),
            pltpu.VMEM((leaf_count, leaf_size, 128), F32),
            pltpu.VMEM((leaf_count, 8, leaf_size), F32),
            pltpu.VMEM((leaf_count, 2 * classes, leaf_size), BF16),
        ],
    )(points, vector, near_mask, *([] if base is None else [base]))


def near_apply(tiles, vector, near_mask, base, first, leaf_count, reach):
    count, leaf_size = tiles.shape[0], tiles.shape[-1]
    classes = vector.shape[0]

    def body(tile_hbm, vector_ref, mask_ref, *refs):
        base_ref = refs[0] if base is not None else None
        out_ref, vecs, tile_ref, sems = refs[-4:]
        def loads(t):
            return [pltpu.make_async_copy(tile_hbm.at[t, e], tile_ref.at[t, e], sems.at[t, e]) for e in range(3)]

        for t in range(count):
            for copy in loads(t):
                copy.start()
        out_ref[...] = jnp.zeros_like(out_ref) if base_ref is None else base_ref[...]
        for j in range(first, min(first + count + 2, leaf_count)):
            vecs[j] = stacked(vector_ref[:, j * leaf_size : (j + 1) * leaf_size])

        @pl.loop(0, count)
        def _(t):
            for copy in loads(t):
                copy.wait()

            near_products(near_pairs(first + t, leaf_count), mask_ref, vecs, tile_ref.at[pl.ds(t, 1)], out_ref, reach)

    return call(
        body,
        struct((leaf_count, classes, leaf_size)),
        "near_apply",
        20,
        in_specs=[HBM, VM, SM] + ([] if base is None else [VM]),
        out_specs=VM,
        scratch_shapes=[
            pltpu.VMEM((leaf_count, 2 * classes, leaf_size), BF16),
            pltpu.VMEM(tiles.shape, BF16),
            pltpu.SemaphoreType.DMA((count, 3)),
        ],
    )(in_hbm(tiles), vector, near_mask, *([] if base is None else [base]))


def edges(leaf_count, reach):
    found = []
    for side in range(2):
        for h in range(reach):
            for j in range(reach):
                own = j if side == 0 else leaf_count - reach + j
                offset = h - reach - own if side == 0 else leaf_count + h - own
                if -reach <= offset <= reach:
                    found.append((side, h, j, own, reach + offset))
    return jnp.array(found, jnp.int32)


def edge_build(points, left, right, near_mask, classes, leaf_count, reach):
    dim = points.shape[1]
    leaf_size = points.shape[0] // leaf_count
    lanes = leaf_size // 128
    width = reach * leaf_size
    border = edges(leaf_count, reach)
    count = border.shape[0]

    def body(own_hbm, left_ref, right_ref, mask_ref, border_ref, tile_hbm, out_ref, tile_ref, own_ref, sems, out_sems):
        halo_refs = (left_ref, right_ref)
        tail = pl.ds((leaf_count - reach) * leaf_size, width)
        loads = [
            pltpu.make_async_copy(src, dst, sems.at[i])
            for i, (src, dst) in enumerate(
                [
                    (own_hbm.at[pl.ds(0, width)], own_ref.at[0]), (own_hbm.at[tail], own_ref.at[1]),
                ]
            )
        ]
        for copy in loads:
            copy.start()
        out_ref[...] = jnp.zeros_like(out_ref)
        for copy in loads:
            copy.wait()

        def cat_of(ref, spot):
            return scaled_cat(ref[pl.ds(pl.multiple_of(spot * leaf_size, leaf_size), leaf_size), :])

        def rows_of(i, spot):
            firsts = [pl.multiple_of(width + (spot * lanes + n) * classes, classes) for n in range(lanes)]
            return jnp.concatenate([halo_refs[i][pl.ds(f, classes), :] for f in firsts], axis=1)

        def store(t):
            return pltpu.make_async_copy(tile_ref.at[t], tile_hbm.at[t], out_sems.at[t])

        @pl.loop(0, count // 2)
        def _(step):
            added = []
            for side in range(2):
                t = step + side * (count // 2)
                h, j, own, slot = [border_ref[t, i] for i in range(1, 5)]
                cat_h, cat_j = cat_of(halo_refs[side], h), cat_of(own_ref.at[side], j)
                tile = pair_tile(cat_h, cat_j, half_norms(cat_h)[0], half_norms(cat_j)[1])
                tile_ref[t, 0], tile_ref[t, 1] = split(tile)
                added.append((side * reach + j, mask_ref[own, slot], stacked(rows_of(side, h)), t))
            for place, mask, rows, t in added:
                apply_tile(mask, rows, tile_ref[t, 0], tile_ref[t, 1], out_ref, place)
                store(t).start()

        @pl.loop(0, count)
        def _(t):
            store(t).wait()

    shape = (count, 2, leaf_size, leaf_size)
    return call(
        body,
        (pltpu.HBM(shape, BF16), struct((2 * reach, classes, leaf_size))),
        "edge_build",
        22,
        in_specs=[HBM, VM, VM, SM, SM],
        out_specs=(HBM, VM),
        scratch_shapes=[
            pltpu.VMEM(shape, BF16),
            pltpu.VMEM((2, width, dim), F32),
            pltpu.SemaphoreType.DMA((2,)),
            pltpu.SemaphoreType.DMA((count,)),
        ],
    )(in_hbm(points), left, right, near_mask, border)


def edge_apply(tiles, left_rows, right_rows, near_mask, leaf_count, reach):
    count, leaf_size = tiles.shape[0], tiles.shape[-1]
    classes = left_rows.shape[0]

    def body(tile_hbm, lv_ref, rv_ref, mask_ref, border_ref, out_ref, tile_ref, vecs, sems):
        def load(t):
            return pltpu.make_async_copy(tile_hbm.at[t], tile_ref.at[t], sems.at[t])

        for step in range(count // 2):
            load(step).start()
            load(step + count // 2).start()
        out_ref[...] = jnp.zeros_like(out_ref)
        for h in range(reach):
            where = slice(h * leaf_size, (h + 1) * leaf_size)
            vecs[0, h] = stacked(lv_ref[:, where])
            vecs[1, h] = stacked(rv_ref[:, where])

        @pl.loop(0, count // 2)
        def _(step):
            load(step).wait()
            load(step + count // 2).wait()
            for side in range(2):
                t = step + side * (count // 2)
                h, j, own, slot = [border_ref[t, i] for i in range(1, 5)]
                apply_tile(
                    mask_ref[own, slot], vecs[side, h], tile_ref[t, 0], tile_ref[t, 1], out_ref, side * reach + j
                )

    return call(
        body,
        struct((2 * reach, classes, leaf_size)),
        "edge_apply",
        14,
        in_specs=[HBM, VM, VM, SM, SM],
        out_specs=VM,
        scratch_shapes=[
            pltpu.VMEM(tiles.shape, BF16),
            pltpu.VMEM((2, reach, 2 * classes, leaf_size), BF16),
            pltpu.SemaphoreType.DMA((count,)),
        ],
    )(in_hbm(tiles), left_rows, right_rows, near_mask, edges(leaf_count, reach))


def tree_stage(device, packs, node_gain, transfer, node_skeleton, classes, leaves, level, bit, with_skel, extra, climb):
    count = len(packs)
    skel_size = packs[0].shape[1]
    levels = count.bit_length() - 1
    skel_rows = skel_size // 2 if with_skel else 0
    out_rows = packs[0].shape[0]

    def body(*refs):
        dev_ref, pack_refs = refs[0], refs[1 : 1 + count]
        rest = list(refs[1 + count :])
        gains_ref, transfer_ref = rest.pop(0), rest.pop(0)
        node_ref = rest.pop(0) if with_skel else None
        sibling_ref = rest.pop(0)
        next_ref = rest.pop(0)
        hi_ref, lo_ref = (rest.pop(0), rest.pop(0)) if with_skel else (None, None)
        joined = rest.pop(0)
        device = dev_ref[0]
        place = lax.shift_right_logical(device, bit) & (count - 1)
        base = lax.shift_right_logical(device, bit + levels)
        if with_skel and (climb or levels > 1):
            rows_ref = rest.pop(0)
            rows_ref[...] = jnp.zeros_like(rows_ref)
            spot = 0
            for depth in range(1, levels + 1 if climb else levels):
                nodes = count >> depth
                row = leaves - 2 * (leaves >> (level + depth)) + base * nodes
                for i in range(nodes):
                    rows_ref[spot : spot + 1, :] = node_ref[pl.ds(row + i, 1), :]
                    spot += 1
            pick_columns = columns(rows_ref[...])
        for i in range(count):
            joined[place ^ i] = pack_refs[i][...]
        weights = [joined[i][:classes] for i in range(count)]
        skels = []
        if with_skel:
            skels = [
                jnp.concatenate(split(unpack_skel(joined[i][classes : classes + skel_rows])), axis=1)
                for i in range(count)
            ]
        pick_first = 0
        for depth in range(levels):
            own = lax.shift_right_logical(place, depth)
            other = own ^ 1
            chosen = weights[0]
            for i in range(1, len(weights)):
                chosen = jnp.where(other == i, weights[i], chosen)
            sibling_ref[depth] = chosen
            if with_skel:
                mine, theirs = skels[0], skels[0]
                for i in range(1, len(skels)):
                    mine = jnp.where(own == i, skels[i], mine)
                    theirs = jnp.where(other == i, skels[i], theirs)
                tile = pair_tile(theirs, mine, half_norms(theirs)[0], half_norms(mine)[1])
                hi_ref[depth], lo_ref[depth] = split(tile)
            if depth + 1 < levels or climb:
                row = 2 * leaves - 2 * (leaves >> (level + depth)) + base * len(weights)
                scaled = [w * gains_ref[pl.ds(row + i, 1), :] for i, w in enumerate(weights)]
                left = times(stacked(jnp.concatenate(scaled[0::2], axis=0)), *split(transfer_ref[depth, 0]))
                right = times(stacked(jnp.concatenate(scaled[1::2], axis=0)), *split(transfer_ref[depth, 1]))
                total = left + right
                weights = [total[i * classes : (i + 1) * classes] for i in range(len(weights) // 2)]
                if with_skel:
                    above = []
                    for p in range(len(skels) // 2):
                        both = jnp.concatenate([skels[2 * p], skels[2 * p + 1]], axis=0)
                        pick = one_hot(pick_columns[:, pick_first : pick_first + 1], 2 * skel_size)
                        above.append(nn(pick, both).astype(BF16))
                        pick_first += 1
                    skels = above
        if climb:
            next_ref[:classes] = weights[0]
            if with_skel:
                dim = skels[0].shape[1] // 2
                pack_skel(next_ref, classes, skels[0][:, :dim].astype(F32) + skels[0][:, dim:].astype(F32))
        else:
            next_ref[: classes + skel_rows] = jnp.zeros((classes + skel_rows, skel_size), F32)
        if extra:
            rows = slice(classes + skel_rows, out_rows)
            total = joined[0][rows]
            for i in range(1, count):
                total = total + joined[i][rows]
            next_ref[rows] = total

    out = [struct((levels, classes, skel_size)), struct((out_rows, skel_size))]
    if with_skel:
        out += [struct((levels, skel_size, skel_size), BF16)] * 2
    scratch = [pltpu.VMEM((count, out_rows, skel_size), F32)]
    ins = [device, *packs, node_gain, transfer]
    if with_skel:
        ins.append(node_skeleton)
        if climb or levels > 1:
            scratch.append(pltpu.VMEM((8, skel_size), jnp.int32))
    return call(
        body,
        tuple(out),
        "tree_stage",
        10,
        in_specs=[SM] + [VM] * (len(ins) - 1),
        out_specs=tuple([VM] * len(out)),
        scratch_shapes=scratch,
    )(*ins)


def downward(
    device, vector, near, edge, leaf_interp, transfer, local_weights, local_tiles, node_gain,
    siblings, device_tiles, reach, leaves, start,
):
    leaf_count, leaf_size, skel_size = leaf_interp.shape
    classes = vector.shape[0]
    local_levels = leaf_count.bit_length() - 1
    stages = len(siblings)

    def body(*refs):
        dev_ref, vector_ref, near_ref, edge_ref, interp_ref, maps_ref = refs[:6]
        weights_ref, tiles_hi, tiles_lo, gain_ref = refs[6:10]
        sib_refs = refs[10 : 10 + stages]
        dev_refs = refs[10 + stages : 10 + 3 * stages]
        rest = list(refs[10 + 3 * stages :])
        device = dev_ref[0]

        def gain(level, node):
            return gain_ref[pl.ds(2 * leaves - 2 * (leaves >> level) + node, 1), :]

        image_ref = rest.pop(0)
        head_ref, tail_ref = (rest.pop(0), rest.pop(0)) if start else (None, None)
        gram_ref = rest.pop(0) if start else None
        local = []
        for s in range(stages):
            for i in range(sib_refs[s].shape[0]):
                local.append(times(stacked(sib_refs[s][i]), dev_refs[2 * s][i], dev_refs[2 * s + 1][i]))
        top = len(local) - 1
        potential = local[top]
        for b in range(top - 1, -1, -1):
            node = lax.shift_right_logical(device, b)
            down = maps_ref[local_levels + b, node & 1]
            potential = times(stacked(potential), *split(down), nt) * gain(local_levels + b, node) + local[b]
        level = [potential]
        for depth in range(local_levels - 1, -1, -1):
            cat = stacked(jnp.concatenate(level, axis=0))
            sides = [times(cat, *split(maps_ref[depth, c]), nt) for c in range(2)]
            count = leaf_count >> depth
            first = 2 * leaf_count - 2 * count
            pair_first = leaf_count - count
            below = []
            for n in range(count):
                p, c = n // 2, n % 2
                cat_sibling = stacked(weights_ref[first + (n ^ 1)])
                hi, lo = tiles_hi[pair_first + p], tiles_lo[pair_first + p]
                direct = times(cat_sibling, hi, lo, nn if c else nt)
                carried = sides[c][p * classes : (p + 1) * classes]
                below.append(carried * gain(depth, device * count + n) + direct)
            level = below
        for j in range(leaf_count):
            where = slice(j * leaf_size, (j + 1) * leaf_size)
            total = ridge * vector_ref[:, where] + near_ref[j]
            if j < reach:
                total = total + edge_ref[j]
            if j >= leaf_count - reach:
                total = total + edge_ref[reach + j - (leaf_count - reach)]
            image_ref[:, where] = total + times(stacked(level[j]), *split(interp_ref[j]), nt)
        if start:
            width = reach * leaf_size
            head_ref[...] = image_ref[:, :width]
            tail_ref[...] = image_ref[:, (leaf_count - reach) * leaf_size :]
            whole = nt(stacked(vector_ref[...]), jnp.concatenate([stacked(vector_ref[...]), stacked(image_ref[...])], axis=0))
            half = whole[:classes] + whole[classes:]
            rows = classes // 2
            self_gram = half[:, :classes] + half[:, classes : 2 * classes]
            image_gram = half[:, 2 * classes : 3 * classes] + half[:, 3 * classes :]
            gram = jnp.concatenate([self_gram, image_gram], axis=1)
            gram_ref[:, : 2 * classes] = gram[:rows]
            gram_ref[:, 2 * classes :] = gram[rows:]

    out = [struct(vector.shape)]
    if start:
        out += [struct((classes, reach * leaf_size))] * 2
        out.append(struct((classes // 2, 4 * classes)))
    ins = [device, vector, near, edge, leaf_interp, transfer, local_weights, *local_tiles, node_gain]
    ins += list(siblings)
    for pair in device_tiles:
        ins += list(pair)
    specs = [SM] + [VM] * (len(ins) - 1)
    return call(
        body,
        tuple(out),
        "downward",
        30,
        in_specs=specs,
        out_specs=tuple([VM] * len(out)),
    )(*ins)


def mixed(matrix, rows):
    m_hi, m_lo = split(matrix)
    r_hi, r_lo = split(rows)
    return nn(
        jnp.concatenate([m_hi, m_lo, m_hi, m_lo], axis=1),
        jnp.concatenate([r_hi, r_hi, r_lo, r_lo], axis=0),
    )


def three(x):
    hi = x.astype(BF16)
    rest = x - hi.astype(F32)
    mid = rest.astype(BF16)
    return hi, mid, (rest - mid.astype(F32)).astype(BF16)


def exact_dot(a, b):
    a0, a1, a2 = three(a)
    b0, b1, b2 = three(b)
    return nn(
        jnp.concatenate([a2, a1, a0, a1, a0, a0], axis=1),
        jnp.concatenate([b0, b1, b2, b0, b1, b0], axis=0),
    )


def eliminate(systems, width=4):
    size, wide = systems[0].shape
    place = lax.broadcasted_iota(jnp.int32, (size, wide), 0)
    for first in range(0, size, width):
        block = [
            [jnp.broadcast_to(m[:, k : k + 1], (size, wide)) for k in range(first, first + width)]
            for m in systems
        ]
        for i in range(width):
            k = first + i
            pivot = place == k
            for n in range(len(systems)):
                cols = block[n]
                inverse = 1.0 / cols[i][k : k + 1, :]
                for j in range(i + 1, width):
                    scaled = cols[j][k : k + 1, :] * inverse
                    cols[j] = jnp.where(pivot, scaled, cols[j] - cols[i] * scaled)
                scaled = systems[n][k : k + 1, :] * inverse
                systems[n] = jnp.where(pivot, scaled, systems[n] - cols[i] * scaled)
    return systems


def first_step(gram, right_side, image, second):
    classes = right_side.shape[0]

    def body(gram_in, b_ref, image_ref, second_ref, res_ref, res_image_ref, gram_ref, alpha_ref, both_ref):
        packed = gram_in[classes:, :]
        both = jnp.concatenate([packed[:, : 2 * classes], packed[:, 2 * classes :]], axis=0)
        turned = both.T
        base = 0.5 * (both[:, :classes] + turned[:classes])
        curvature = 0.5 * (both[:, classes:] + turned[classes:])
        (solved,) = eliminate([jnp.concatenate([curvature, base], axis=1)])
        alpha_t = solved.T[classes:]
        alpha_ref[...] = alpha_t
        both_ref[...] = both
        res = b_ref[...] - mixed(alpha_t, image_ref[...])
        res_image = image_ref[...] - mixed(alpha_t, second_ref[...])
        res_ref[...] = res
        res_image_ref[...] = res_image
        res_cat, base_cat = stacked(res), stacked(b_ref[...])
        left = jnp.concatenate([res_cat, base_cat], axis=0)
        right = jnp.concatenate([res_cat, stacked(res_image), stacked(image_ref[...])], axis=0)
        whole = nt(left, right)

        def block(i, j):
            part = whole[2 * i * classes : 2 * (i + 1) * classes, 2 * j * classes : 2 * (j + 1) * classes]
            half = part[:classes] + part[classes:]
            return half[:, :classes] + half[:, classes:]

        gram_ref[...] = jnp.concatenate([block(0, 0), block(0, 1), block(0, 2), block(1, 1)], axis=1)

    return call(
        body,
        (
            struct(right_side.shape),
            struct(right_side.shape),
            struct((classes, 4 * classes)),
            struct((classes, classes)),
            struct((classes, 2 * classes)),
        ),
        "first_step",
        28,
    )(gram, right_side, image, second)


def between(both, alpha_t, right_side):
    classes = right_side.shape[0]

    def body(both_ref, alpha_ref, b_ref, inverse_ref, moved_ref):
        both = both_ref[...]
        base = 0.5 * (both[:, :classes] + both.T[:classes])
        square = (classes, classes)
        unit = jnp.where(
            lax.broadcasted_iota(jnp.int32, square, 0) == lax.broadcasted_iota(jnp.int32, square, 1), 1.0, 0.0
        )
        (inverse,) = eliminate([jnp.concatenate([base, unit], axis=1)])
        inverse_ref[...] = inverse[:, classes:]
        moved_ref[...] = mixed(alpha_ref[...], b_ref[...])

    return call(body, (struct((classes, classes)), struct(right_side.shape)), "between", 16)(
        both, alpha_t, right_side
    )


def last_step(both, inverse, moved, parts, right_side, image, res, res_image):
    classes = right_side.shape[0]
    count = len(parts)

    def body(both_ref, inverse_ref, moved_ref, *refs):
        base_ref, image_ref, res_ref, res_image_ref, sol_ref, out_ref = refs[count:]
        grams = [ref[...] for ref in refs[:count]]
        while len(grams) > 1:
            grams = [a + b for a, b in zip(grams[0::2], grams[1::2])]
        grams = grams[0]
        inverse = inverse_ref[...]
        image_gram = both_ref[:, classes:]
        new_gram = grams[:, :classes]
        new_gram = 0.5 * (new_gram + grams[:, : 2 * classes].T[:classes])
        beta = exact_dot(inverse, new_gram)
        beta_t = jnp.concatenate([beta, beta], axis=1).T[:classes]
        res_image_gram = grams[:, classes : 2 * classes]
        res_base = grams[:, 2 * classes : 3 * classes]
        base_res = grams[:, 3 * classes :]
        curvature = (
            res_image_gram
            + exact_dot(res_base, beta)
            + exact_dot(beta_t, base_res + exact_dot(image_gram, beta))
        )
        curvature = 0.5 * (curvature + jnp.concatenate([curvature, curvature], axis=1).T[:classes])
        (solved,) = eliminate([jnp.concatenate([curvature, new_gram], axis=1)])
        alpha2_t = solved.T[classes:]
        direction = res_ref[...] + mixed(beta_t, base_ref[...])
        sol_ref[...] = moved_ref[...] + mixed(alpha2_t, direction)
        direction_image = res_image_ref[...] + mixed(beta_t, image_ref[...])
        out_ref[...] = res_ref[...] - mixed(alpha2_t, direction_image)

    return call(body, (struct(right_side.shape), struct(right_side.shape)), "last_step", 28)(
        both, inverse, moved, *parts, right_side, image, res, res_image
    )


def body(
    points, right_side, neighbours, leaf_interp, leaf_skeleton, node_skeleton, node_gain, transfer
):
    leaf_count, slot_count = neighbours.shape
    reach = (slot_count - 1) // 2
    leaf_size, skel_size = leaf_interp.shape[1:]
    classes = right_side.shape[0]
    dev_count = lax.axis_size("leaf")
    dev_levels = dev_count.bit_length() - 1
    local_levels = leaf_count.bit_length() - 1
    levels = local_levels + dev_levels
    leaves = leaf_count * dev_count
    device = lax.axis_index("leaf").astype(jnp.int32)[None]

    def exchange(head, tail):
        ends = dev_count - 1
        left = lax.ppermute(tail, "leaf", [(i, i + 1) for i in range(ends)])
        right = lax.ppermute(head, "leaf", [(i + 1, i) for i in range(ends)])
        return left, right

    def group(pack, first_bit, count):
        return [pack] + [
            lax.ppermute(pack, "leaf", [(d, d ^ (i << first_bit)) for d in range(dev_count)])
            for i in range(1, count)
        ]

    stages = [(bit, min(2, dev_levels - bit)) for bit in range(0, dev_levels, 2)]
    near_mask = neighbours

    def climb(pack, with_skel, extra, covers):
        siblings, tiles, results = [], [], []
        for stage, (bit, width) in enumerate(stages):
            level = local_levels + bit
            depth = min(width, levels - 1 - level) or 1
            first = min(level, levels - 1 - depth)
            packs = group(pack, bit, 1 << width)
            if stage < len(covers):
                done = covers[stage](pack)
                results.append(done)
                packs, _ = lax.optimization_barrier((packs, done[-1]))
            found = tree_stage(
                device, packs, node_gain, lax.slice_in_dim(transfer, first, first + depth, axis=0),
                node_skeleton, classes, leaves, level, bit, with_skel, extra, level + width < levels,
            )
            siblings.append(found[0])
            pack = found[1]
            if with_skel:
                tiles.append((found[2], found[3]))
        return siblings, tiles, pack, results

    def after(pack, *values):
        return lax.optimization_barrier((pack, values))[1]

    assert reach == 2
    steps = leaf_count - 1
    cuts = [0, -(-steps * 3 // 7), -(-steps * 5 // 7), steps]

    own_skel, *local_tiles, head, tail = front(
        device, points, right_side, leaf_skeleton, node_skeleton, leaf_count, leaves, reach
    )
    left, right = exchange(head, tail)
    near_tiles, total = [], [None]

    def build(part):
        def run(pack):
            (vector,) = after(pack, right_side)
            own_points = points if part else in_hbm(points)
            vector = vector if part else in_hbm(vector)
            tiles, total[0] = near_build(
                own_points, vector, near_mask, total[0], cuts[part], cuts[part + 1] - cuts[part], leaf_count, reach
            )
            near_tiles.append(tiles)
            return total[0],

        return run

    def build_last(pack):
        left_pack, right_pack, _ = after(pack, left, right, total[0])
        return edge_build(points, left_pack, right_pack, near_mask, classes, leaf_count, reach)

    build(0)(own_skel)
    (vector,) = after(total[0], right_side)
    local_transfer = lax.slice_in_dim(transfer, 0, local_levels, axis=0)
    pack, weights = upward(device, vector, own_skel, leaf_interp, local_transfer, node_gain, leaves)
    siblings, device_tiles, _, results = climb(pack, True, False, [build(1), build(2), build_last])
    near = total[0]
    edge_tiles, edge = results[2]
    image, head, tail, gram = downward(
        device, right_side, near, edge, leaf_interp, transfer, weights, local_tiles, node_gain,
        siblings, device_tiles, reach, leaves, True,
    )

    pack, weights = upward(device, image, gram, leaf_interp, local_transfer, node_gain, leaves)
    left_rows, right_rows = exchange(*after(pack, head, tail))
    total = [None]

    def apply(part):
        def run(pack):
            (vector,) = after(pack, image)
            total[0] = near_apply(near_tiles[part], vector, near_mask, total[0], cuts[part], leaf_count, reach)
            return total[0],

        return run

    def apply_last(pack):
        apply(2)(pack)
        left, right, _ = after(pack, left_rows, right_rows, total[0])
        return (edge_apply(edge_tiles, left, right, near_mask, leaf_count, reach),)

    siblings, _, pack, results = climb(pack, False, True, [apply(0), apply(1), apply_last])
    near, (edge,) = total[0], results[2]
    (second,) = downward(
        device, image, near, edge, leaf_interp, transfer, weights, local_tiles, node_gain,
        siblings, device_tiles, reach, leaves, False,
    )

    res, res_image, grams, alpha_t, both = first_step(pack, right_side, image, second)
    inverse, moved = between(both, alpha_t, right_side)
    for stage, (bit, width) in enumerate(stages[:-1]):
        parts = group(grams, bit, 1 << width)
        if stage == 0:
            parts, (inverse, moved) = lax.optimization_barrier((parts, (inverse, moved)))
        while len(parts) > 1:
            parts = [a + b for a, b in zip(parts[0::2], parts[1::2])]
        grams = parts[0]
    bit, width = stages[-1]
    parts = group(grams, bit, 1 << width)
    return last_step(both, inverse, moved, parts, right_side, image, res, res_image)


def solution(mesh):
    placed = (
        P("leaf", None),
        P(None, "leaf"),
        P("leaf", None),
        P("leaf", None, None),
        P("leaf", None),
        P(),
        P(),
        P(),
    )
    return jax.shard_map(
        body,
        mesh=mesh,
        in_specs=placed,
        out_specs=(P(None, "leaf"), P(None, "leaf")),
        check_vma=False,
    )
```
